16 devices in a mesh: dp: 4 (over z, y), emb: 4 (over x, core).
Axes of the slice: x: 2, y: 2, z: 2, core: 2. Of those that a mesh axis runs over, the one named last changes fastest.
Arguments:
- tok_ids: int32 [8192], P(('dp', 'emb'))
- resid_in: bfloat16 [8192, 1024], P(('dp', 'emb'))
- cot_out: bfloat16 [8192, 1024], P(('dp', 'emb'))
- tables: bfloat16 [3, 65536, 1024], P(None, 'emb')
- w_up: bfloat16 [3, 1024, 4096], replicated
- w_down: bfloat16 [3, 4096, 1024], replicated
- w_gate: bfloat16 [3, 1024, 1024], replicated
- w_proj: bfloat16 [3, 1024, 1024], replicated
Outputs:
- output 1: bfloat16 [8192, 1024], P(('dp', 'emb'))
- output 2: float32 [3, 65536, 1024], P(None, 'emb')
All inputs are finite; a program needn't handle non-finite values.
Results may differ from the reference program's by a relative error of at most 0.00918168.
Values are sent between devices in bfloat16 or wider.
A program may use at most 1.5 GiB of HBM per device.

```python
import jax
import jax.numpy as jnp
from jax import lax

TOKENS_DEV = 512
LAYERS = 3
D_MODEL = 1024
FFN_DIM = 4096
EMB_DIM = 1024
VOCAB_SIZE = 65536
NUM_DP = 4
NUM_EMB = 4
CAP_ROWS = 256

N_TOKENS = TOKENS_DEV * NUM_DP * NUM_EMB
RANGE_ROWS = VOCAB_SIZE // NUM_EMB
HOT_SET = min(16, RANGE_ROWS)
NORM_EPS = 1e-6


def draw_ids(id_key):
    key_list = jax.random.split(id_key, 9)
    n_dev = NUM_DP * NUM_EMB
    draw_shape = (n_dev, TOKENS_DEV)
    tok_pos = jnp.arange(TOKENS_DEV, dtype=jnp.int32)[None, :]
    hot_top = jax.random.randint(key_list[0], (n_dev, 1), 1, NUM_EMB + 1)
    hot_owner = jax.random.randint(key_list[1], (n_dev, 1), 0, hot_top)
    shift_by = jax.random.randint(key_list[2], (n_dev, 1), 0, NUM_EMB - 1)
    spread = (hot_owner + 1 + (tok_pos - CAP_ROWS + shift_by) % (NUM_EMB - 1)) % NUM_EMB
    owner_seq = jnp.where(tok_pos < CAP_ROWS, hot_owner, spread)
    scores = jax.random.randint(key_list[3], draw_shape, 0, TOKENS_DEV) * TOKENS_DEV + tok_pos
    perm_order = jnp.argsort(scores, axis=1)
    owner_ids = jnp.take_along_axis(owner_seq, perm_order, axis=1)
    is_hot = jax.random.randint(key_list[4], draw_shape, 0, 4) == 0
    hot_off = jax.random.randint(key_list[5], draw_shape, 0, HOT_SET)
    span_a = jax.random.randint(key_list[6], draw_shape, 1, RANGE_ROWS + 1)
    span_b = jax.random.randint(key_list[7], draw_shape, 1, span_a + 1)
    tail_off = jax.random.randint(key_list[8], draw_shape, 0, span_b)
    offset = jnp.where(is_hot, hot_off, tail_off)
    return (owner_ids * RANGE_ROWS + offset).reshape(-1).astype(jnp.int32)


def setup_inputs(seed: int = 0) -> dict:
    root_key = jax.random.key(seed)
    key_list = jax.random.split(root_key, 8)
    tok_ids = draw_ids(key_list[0])
    resid_in = jax.random.normal(key_list[1], (N_TOKENS, D_MODEL), jnp.float32).astype(jnp.bfloat16)
    cot_out = jax.random.normal(key_list[2], (N_TOKENS, D_MODEL), jnp.float32).astype(jnp.bfloat16)
    tables = (0.5 * jax.random.normal(key_list[3], (LAYERS, VOCAB_SIZE, EMB_DIM), jnp.float32)).astype(jnp.bfloat16)
    w_up = (jax.random.normal(key_list[4], (LAYERS, D_MODEL, FFN_DIM), jnp.float32) * D_MODEL ** -0.5).astype(jnp.bfloat16)
    w_down = (jax.random.normal(key_list[5], (LAYERS, FFN_DIM, D_MODEL), jnp.float32) * (0.5 * FFN_DIM ** -0.5)).astype(jnp.bfloat16)
    w_gate = (jax.random.normal(key_list[6], (LAYERS, D_MODEL, EMB_DIM), jnp.float32) * D_MODEL ** -0.5).astype(jnp.bfloat16)
    w_proj = (jax.random.normal(key_list[7], (LAYERS, EMB_DIM, D_MODEL), jnp.float32) * EMB_DIM ** -0.5).astype(jnp.bfloat16)
    return {'tok_ids': tok_ids, 'resid_in': resid_in, 'cot_out': cot_out, 'tables': tables, 'w_up': w_up, 'w_down': w_down, 'w_gate': w_gate, 'w_proj': w_proj}


def rms_norm(x_f32):
    return x_f32 * lax.rsqrt(jnp.mean(x_f32 * x_f32, axis=-1, keepdims=True) + NORM_EPS)


def layer_forward(resid_cur, fetched, w_up_l, w_down_l, w_gate_l, w_proj_l):
    x_f32 = resid_cur.astype(jnp.float32)
    normed = rms_norm(x_f32).astype(jnp.bfloat16)
    hidden = jax.nn.gelu(jnp.dot(normed, w_up_l, preferred_element_type=jnp.float32)).astype(jnp.bfloat16)
    mlp_out = jnp.dot(hidden, w_down_l, preferred_element_type=jnp.float32)
    gate_act = jax.nn.gelu(jnp.dot(normed, w_gate_l, preferred_element_type=jnp.float32))
    mixed_in = (gate_act * fetched).astype(jnp.bfloat16)
    proj_out = jnp.dot(mixed_in, w_proj_l, preferred_element_type=jnp.float32)
    return (x_f32 + mlp_out + proj_out).astype(jnp.bfloat16)


def reference(tok_ids, resid_in, cot_out, tables, w_up, w_down, w_gate, w_proj):
    def fwd_step(resid_cur, layer_params):
        table_l, w_up_l, w_down_l, w_gate_l, w_proj_l = layer_params
        fetched = jnp.take(table_l, tok_ids, axis=0).astype(jnp.float32)
        resid_next = layer_forward(resid_cur, fetched, w_up_l, w_down_l, w_gate_l, w_proj_l)
        return resid_next, resid_cur

    resid_out, resid_saved = lax.scan(fwd_step, resid_in, (tables, w_up, w_down, w_gate, w_proj))

    def bwd_step(cot_next, layer_params):
        resid_cur, table_l, w_up_l, w_down_l, w_gate_l, w_proj_l = layer_params
        fetched = jnp.take(table_l, tok_ids, axis=0).astype(jnp.float32)

        def local_layer(resid_arg, fetched_arg):
            return layer_forward(resid_arg, fetched_arg, w_up_l, w_down_l, w_gate_l, w_proj_l)

        pullback = jax.vjp(local_layer, resid_cur, fetched)[1]
        cot_cur, d_fetched = pullback(cot_next)
        d_table = jax.ops.segment_sum(d_fetched, tok_ids, num_segments=VOCAB_SIZE)
        return cot_cur, d_table

    cot_first, d_tables = lax.scan(bwd_step, cot_out, (resid_saved, tables, w_up, w_down, w_gate, w_proj), reverse=True)
    return resid_out, d_tables
```

```python
import functools

import jax
import jax.numpy as jnp
from jax import lax
from jax.experimental import pallas as pl
from jax.experimental.pallas import tpu as pltpu
from jax.sharding import PartitionSpec as P


NORM_EPS = 1e-6
BF = jnp.bfloat16
F32 = jnp.float32

CHUNK = 16
BLK = 256
TILE_ROWS = 1024


def rms_norm(x_f32):
    return x_f32 * lax.rsqrt(jnp.mean(x_f32 * x_f32, axis=-1, keepdims=True) + NORM_EPS)


def layer_forward(x, normed, fetched, w_up, w_down, w_gate, w_proj):
    x_f32 = x.astype(F32)
    up_pre = jnp.dot(normed, w_up, preferred_element_type=F32)
    hidden = jax.nn.gelu(up_pre).astype(BF)
    mlp_out = jnp.dot(hidden, w_down, preferred_element_type=F32)
    gate_pre = jnp.dot(normed, w_gate, preferred_element_type=F32)
    gate_act = jax.nn.gelu(gate_pre)
    mixed_in = (gate_act * fetched.astype(F32)).astype(BF)
    proj_out = jnp.dot(mixed_in, w_proj, preferred_element_type=F32)
    x_next = (x_f32 + mlp_out + proj_out).astype(BF)
    return x_next, (x, up_pre, gate_pre, fetched)


def mixed_cot(cot_next, w_proj):
    return jnp.einsum('td,ed->te', cot_next, w_proj, preferred_element_type=F32).astype(BF)


def layer_backward(cot_next, d_mixed, saved, w_up, w_down, w_gate):
    x, up_pre, gate_pre, fetched = saved
    d_gate_act = d_mixed.astype(F32) * fetched.astype(F32)
    d_gate_pre = jax.vjp(jax.nn.gelu, gate_pre)[1](d_gate_act)[0]
    d_hidden = jnp.einsum('td,fd->tf', cot_next, w_down, preferred_element_type=F32).astype(BF)
    d_up_pre = jax.vjp(jax.nn.gelu, up_pre)[1](d_hidden.astype(F32))[0]
    d_norm_mlp = jnp.einsum('tf,df->td', d_up_pre.astype(BF), w_up, preferred_element_type=F32).astype(BF)
    d_norm_gate = jnp.einsum('te,de->td', d_gate_pre.astype(BF), w_gate, preferred_element_type=F32).astype(BF)
    d_normed = (d_norm_mlp + d_norm_gate).astype(F32)
    d_x_norm = jax.vjp(rms_norm, x.astype(F32))[1](d_normed)[0]
    return (cot_next.astype(F32) + d_x_norm).astype(BF)


def serve_kernel(n_layers, cap, cnt_ref, start_ref, ids_ref, tables, out_ref, blocks, tmp, rows, sem):
    n_emb = out_ref.shape[0]
    groups = [(l, e) for l in range(n_layers) for e in range(n_emb)]

    def copy_of(l, slot, row, buf):
        return pltpu.make_async_copy(
            tables.at[l, pl.ds(pl.multiple_of(row, 8), 8), :], blocks.at[buf, slot], sem.at[buf])

    def issue(g):
        l, e = groups[g]

        def body(s, _):
            row = ids_ref[start_ref[e] + s]
            copy_of(l, s, lax.div(row, 8) * 8, g % 2).start()
            return 0

        lax.fori_loop(0, cnt_ref[e], body, 0)

    issue(0)
    for g, (l, e) in enumerate(groups):
        buf = g % 2
        if g + 1 < len(groups):
            issue(g + 1)
        cnt = cnt_ref[e]

        def drain(s, _):
            copy_of(l, 0, 0, buf).wait()
            return 0

        lax.fori_loop(0, cnt, drain, 0)
        rows[...] = jnp.zeros_like(rows)

        def take(s4, _):
            for u in range(4):
                s = jnp.minimum(s4 * 4 + u, cnt - 1)
                q = lax.rem(ids_ref[start_ref[e] + s], 8)
                val = blocks[buf, s].astype(F32)
                for j in range(8):
                    tmp[pl.ds(u * 64 + j * 8, 8), :] = val[:, j * 128:(j + 1) * 128]
                rows[pl.ds(pl.multiple_of(s * 8, 8), 8), :] = tmp[pl.ds(u * 64 + q, 8, stride=8), :]
            return 0

        lax.fori_loop(0, lax.div(cnt + 3, 4), take, 0)
        for j in range(8):
            out_ref[e, l * cap:(l + 1) * cap, j * 128:(j + 1) * 128] = rows[pl.ds(j, cap, stride=8), :].astype(BF)


def serve_rows(tables, counts, starts, local_ids, cap):
    n_layers, _, width = tables.shape
    n_emb = counts.shape[0]
    smem = pl.BlockSpec(memory_space=pltpu.SMEM)
    return pl.pallas_call(
        functools.partial(serve_kernel, n_layers, cap),
        out_shape=jax.ShapeDtypeStruct((n_emb, n_layers * cap, width), BF),
        in_specs=[smem, smem, smem, pl.BlockSpec(memory_space=pl.ANY)],
        out_specs=pl.BlockSpec(memory_space=pltpu.VMEM),
        scratch_shapes=[
            pltpu.VMEM((2, cap, 8, width), BF),
            pltpu.VMEM((256, 128), F32),
            pltpu.VMEM((cap * 8, 128), F32),
            pltpu.SemaphoreType.DMA((2,)),
        ],
        compiler_params=pltpu.CompilerParams(vmem_limit_bytes=40 << 20),
        cost_estimate=pl.CostEstimate(flops=20_000_000_000, bytes_accessed=30_000_000, transcendentals=0),
        name="serve_rows",
    )(counts, starts, local_ids, tables)


def owner_kernel(layer, meta_ref, bound_ref, ids_ref, u_hbm, d_hbm, w_ref, *rest):
    out, uc, dc, prod, acc, sem_u, sem_d, sem_o = rest[-8:]
    n_src = 16
    tile_rows = TILE_ROWS
    n_tiles = bound_ref.shape[0] // n_src - 1
    src_rows = u_hbm.shape[0] // n_src

    def pull(src, dst, sem):
        def run(k, _):
            lo, off = meta_ref[k], meta_ref[2 * n_src + k]

            def chunk(c, _):
                a = pl.multiple_of(k * src_rows + lo + c * CHUNK, CHUNK)
                b = pl.multiple_of((off + c) * CHUNK, CHUNK)
                pltpu.make_async_copy(src.at[pl.ds(a, CHUNK), :], dst.at[pl.ds(b, CHUNK), :], sem).start()
                return 0

            return lax.fori_loop(0, meta_ref[n_src + k], chunk, 0)

        lax.fori_loop(0, n_src, run, 0)

    def drain(src, dst, sem):
        def one(c, _):
            pltpu.make_async_copy(src.at[pl.ds(0, CHUNK), :], dst.at[pl.ds(0, CHUNK), :], sem).wait()
            return 0

        lax.fori_loop(0, meta_ref[3 * n_src], one, 0)

    pull(u_hbm, uc, sem_u)
    pull(d_hbm, dc, sem_d)
    drain(u_hbm, uc, sem_u)
    drain(d_hbm, dc, sem_d)

    def block(b, _):
        r0 = pl.multiple_of(b * BLK, BLK)
        u = uc[pl.ds(r0, BLK), :]
        for n in range(4):
            pre = jnp.dot(u, w_ref[:, n * 256:(n + 1) * 256], preferred_element_type=F32)
            val = jax.nn.gelu(pre) * dc[pl.ds(r0, BLK), n * 256:(n + 1) * 256].astype(F32)
            for j in range(2):
                col = n * 2 + j
                for t in range(BLK // 8):
                    prod[pl.ds(pl.multiple_of(b * (BLK * 8) + t * 64 + col * 8, 8), 8), :] = (
                        val[t * 8:(t + 1) * 8, j * 128:(j + 1) * 128])
        return 0

    lax.fori_loop(0, lax.div(meta_ref[3 * n_src] * CHUNK + BLK - 1, BLK), block, 0)

    def out_copy(t, buf):
        return pltpu.make_async_copy(
            acc.at[buf].reshape(tile_rows // 8, 8, 8, 128),
            out.at[layer, pl.ds(t * (tile_rows // 8), tile_rows // 8)], sem_o.at[buf])

    def tile(t, _):
        buf = lax.rem(t, 2)

        @pl.when(t >= 2)
        def _():
            out_copy(t - 2, buf).wait()

        def clear(i, _):
            base = pl.multiple_of(i * 512, 512)
            acc[buf, pl.ds(base, 512), :] = jnp.zeros((512, 128), F32)
            return 0

        lax.fori_loop(0, tile_rows * 8 // 512, clear, 0)
        row0 = meta_ref[3 * n_src + 1] + t * tile_rows

        def run(k, _):
            first = bound_ref[k * (n_tiles + 1) + t]
            last = bound_ref[k * (n_tiles + 1) + t + 1]
            shift = meta_ref[2 * n_src + k] * CHUNK - meta_ref[k]

            def one(i, _):
                r = ids_ref[k * src_rows + i] - row0
                p = i + shift
                ra = lax.shift_right_logical(r, 3) * 64 + lax.bitwise_and(r, 7)
                pa = lax.shift_right_logical(p, 3) * 64 + lax.bitwise_and(p, 7)
                acc[buf, pl.ds(ra, 8, stride=8), :] += prod[pl.ds(pa, 8, stride=8), :]
                return 0

            return lax.fori_loop(first, last, one, 0)

        lax.fori_loop(0, n_src, run, 0)
        out_copy(t, buf).start()
        return 0

    lax.fori_loop(0, n_tiles, tile, 0)
    out_copy(n_tiles - 2, n_tiles % 2).wait()
    out_copy(n_tiles - 1, (n_tiles - 1) % 2).wait()


def owner_grad(layer, out_prev, out_shape, meta, bounds, ids, u_all, d_all, w_gate):
    smem = pl.BlockSpec(memory_space=pltpu.SMEM)
    hbm = pl.BlockSpec(memory_space=pl.ANY)
    width = w_gate.shape[0]
    max_rows = 17 * BLK
    args = [meta, bounds, ids, u_all, d_all, w_gate]
    specs = [smem, smem, smem, hbm, hbm, pl.BlockSpec(memory_space=pltpu.VMEM)]
    aliases = {}
    if out_prev is not None:
        args.append(out_prev)
        specs.append(hbm)
        aliases = {6: 0}
    return pl.pallas_call(
        functools.partial(owner_kernel, layer),
        out_shape=jax.ShapeDtypeStruct(out_shape, F32),
        in_specs=specs,
        out_specs=hbm,
        scratch_shapes=[
            pltpu.VMEM((max_rows, width), BF),
            pltpu.VMEM((max_rows, width), BF),
            pltpu.VMEM((max_rows * 8, 128), F32),
            pltpu.VMEM((2, TILE_ROWS * 8, 128), F32),
            pltpu.SemaphoreType.DMA,
            pltpu.SemaphoreType.DMA,
            pltpu.SemaphoreType.DMA((2,)),
        ],
        input_output_aliases=aliases,
        compiler_params=pltpu.CompilerParams(vmem_limit_bytes=58 << 20),
        cost_estimate=pl.CostEstimate(flops=40_000_000_000, bytes_accessed=100_000_000, transcendentals=0),
    )(*args)


def solution(mesh):
    n_emb = mesh.shape['emb']
    n_dev = n_emb * mesh.shape['dp']
    tok_spec = P(('dp', 'emb'))
    act_spec = P(('dp', 'emb'), None)
    table_spec = P(None, 'emb', None)
    full_spec = P(None, None, None)
    everyone = ('dp', 'emb')

    def device_body(tok_ids, resid_in, cot_out, tables, w_up, w_down, w_gate, w_proj):
        n_layers, range_rows, _ = tables.shape
        n_tok = tok_ids.shape[0]
        cap = min(2 * n_tok // n_emb, 3 * n_tok // 4)
        i_dp, i_emb = lax.axis_index('dp'), lax.axis_index('emb')

        pos = jnp.arange(n_tok, dtype=jnp.int32)
        before = (tok_ids[None, :] < tok_ids[:, None]) | ((tok_ids[None, :] == tok_ids[:, None]) & (pos[None, :] < pos[:, None]))
        rank = jnp.sum(before.astype(jnp.int32), axis=1)
        perm_mask = rank[None, :] == pos[:, None]
        perm = perm_mask.astype(BF)
        ids = jnp.sum(jnp.where(perm_mask, tok_ids[None, :], 0), axis=1)
        ids_all = lax.all_gather(ids, everyone, axis=0, tiled=True)
        ids_2d = ids_all.reshape(n_dev, n_tok)

        x = jnp.dot(perm, resid_in, preferred_element_type=F32).astype(BF)
        cot = jnp.dot(perm, cot_out, preferred_element_type=F32).astype(BF)

        n_tiles = range_rows // TILE_ROWS
        base = i_emb * range_rows
        edges = base + jnp.arange(n_tiles + 1, dtype=jnp.int32) * TILE_ROWS
        bounds = jnp.sum((ids_2d[:, None, :] < edges[None, :, None]).astype(jnp.int32), axis=2)
        lo = bounds[:, 0]
        hi = bounds[:, n_tiles]
        lo16 = (lo // CHUNK) * CHUNK
        n_ch = (hi - lo16 + CHUNK - 1) // CHUNK
        tri = jnp.arange(n_dev)[None, :] < jnp.arange(n_dev)[:, None]
        off = jnp.sum(jnp.where(tri, n_ch[None, :], 0), axis=1)
        meta = jnp.concatenate([lo16, n_ch, off, jnp.stack([jnp.sum(n_ch), base])]).astype(jnp.int32)

        mine = lax.dynamic_slice(ids_2d, (i_dp * n_emb, 0), (n_emb, n_tok))
        peer_lo = jnp.sum((mine < base).astype(jnp.int32), axis=1)
        peer_hi = jnp.sum((mine < base + range_rows).astype(jnp.int32), axis=1)
        served = serve_rows(tables, peer_hi - peer_lo, peer_lo + jnp.arange(n_emb, dtype=jnp.int32) * n_tok,
                            mine.reshape(-1) - base, cap)
        returned = lax.all_to_all(served, 'emb', 0, 0, tiled=True)
        returned = returned.reshape(n_emb, n_layers, cap, -1)
        owner = ids // range_rows
        first = jnp.sum((owner[None, :] < owner[:, None]).astype(jnp.int32), axis=1)
        slot = owner * cap + pos - first
        pick = (slot[:, None] == jnp.arange(n_emb * cap, dtype=jnp.int32)[None, :]).astype(BF)

        def gather(rows):
            return lax.all_gather(rows, everyone, axis=0, tiled=True)

        last = n_layers - 1
        u_all, saved = [], []
        d_all = [None] * n_layers
        normed = rms_norm(x.astype(F32)).astype(BF)
        u_all.append(gather(normed))
        d_mixed = mixed_cot(cot, w_proj[last])
        d_all[last] = gather(d_mixed)
        for l in range(n_layers):
            rows_l = returned[:, l].reshape(n_emb * cap, -1)
            fetched = jnp.dot(pick, rows_l, preferred_element_type=F32).astype(BF)
            x, kept = layer_forward(x, normed, fetched, w_up[l], w_down[l], w_gate[l], w_proj[l])
            saved.append(kept)
            if l < last:
                normed = rms_norm(x.astype(F32)).astype(BF)
                u_all.append(gather(normed))
        resid_out = lax.dot_general(perm, x, (((0,), (0,)), ((), ())), preferred_element_type=F32).astype(BF)
        for l in range(last, 0, -1):
            cot = layer_backward(cot, d_mixed, saved[l], w_up[l], w_down[l], w_gate[l])
            d_mixed = mixed_cot(cot, w_proj[l - 1])
            d_all[l - 1] = gather(d_mixed)

        width = tables.shape[2]
        grads = None
        out_shape = (n_layers, range_rows // 8, width // 128, 8, 128)
        for l in range(last, -1, -1):
            grads = owner_grad(l, grads, out_shape, meta, bounds.reshape(-1), ids_all, u_all[l], d_all[l], w_gate[l])
        d_tables = grads.transpose(0, 1, 3, 2, 4).reshape(n_layers, range_rows, width)
        return resid_out, d_tables

    return jax.shard_map(device_body, mesh=mesh, in_specs=(tok_spec, act_spec, act_spec, table_spec, full_spec, full_spec, full_spec, full_spec), out_specs=(act_spec, table_spec), check_vma=False)
```

```python
import functools

import jax
import jax.numpy as jnp
from jax import lax
from jax.experimental import pallas as pl
from jax.experimental.pallas import tpu as pltpu
from jax.sharding import PartitionSpec as P


NORM_EPS = 1e-6
BF = jnp.bfloat16
F32 = jnp.float32

CHUNK = 16
BLK = 256
TILE_ROWS = 1024


def rms_norm(x_f32):
    return x_f32 * lax.rsqrt(jnp.mean(x_f32 * x_f32, axis=-1, keepdims=True) + NORM_EPS)


def layer_forward(x, normed, fetched, w_up, w_down, w_gate, w_proj):
    x_f32 = x.astype(F32)
    up_pre = jnp.dot(normed, w_up, preferred_element_type=F32)
    hidden = jax.nn.gelu(up_pre).astype(BF)
    mlp_out = jnp.dot(hidden, w_down, preferred_element_type=F32)
    gate_pre = jnp.dot(normed, w_gate, preferred_element_type=F32)
    gate_act = jax.nn.gelu(gate_pre)
    mixed_in = (gate_act * fetched.astype(F32)).astype(BF)
    proj_out = jnp.dot(mixed_in, w_proj, preferred_element_type=F32)
    x_next = (x_f32 + mlp_out + proj_out).astype(BF)
    return x_next, (x, up_pre, gate_pre, fetched)


def mixed_cot(cot_next, w_proj):
    return jnp.einsum('td,ed->te', cot_next, w_proj, preferred_element_type=F32).astype(BF)


def layer_backward(cot_next, d_mixed, saved, w_up, w_down, w_gate):
    x, up_pre, gate_pre, fetched = saved
    d_gate_act = d_mixed.astype(F32) * fetched.astype(F32)
    d_gate_pre = jax.vjp(jax.nn.gelu, gate_pre)[1](d_gate_act)[0]
    d_hidden = jnp.einsum('td,fd->tf', cot_next, w_down, preferred_element_type=F32).astype(BF)
    d_up_pre = jax.vjp(jax.nn.gelu, up_pre)[1](d_hidden.astype(F32))[0]
    d_norm_mlp = jnp.einsum('tf,df->td', d_up_pre.astype(BF), w_up, preferred_element_type=F32).astype(BF)
    d_norm_gate = jnp.einsum('te,de->td', d_gate_pre.astype(BF), w_gate, preferred_element_type=F32).astype(BF)
    d_normed = (d_norm_mlp + d_norm_gate).astype(F32)
    d_x_norm = jax.vjp(rms_norm, x.astype(F32))[1](d_normed)[0]
    return (cot_next.astype(F32) + d_x_norm).astype(BF)


PICK = 32


def serve_kernel(n_layers, cap, cnt_ref, row_ref, pick_ref, tables, out_ref, blocks, sem):
    n_emb = out_ref.shape[0]

    def issue(e):
        def body(s, _):
            row = pl.multiple_of(row_ref[e * cap + s], 8)
            slot = pl.multiple_of(s * 8, 8)
            pltpu.make_async_copy(
                tables.at[:, pl.ds(row, 8), :], blocks.at[e % 2, :, pl.ds(slot, 8), :], sem.at[e % 2]).start()
            return 0

        lax.fori_loop(0, cnt_ref[e] * PICK, body, 0)

    issue(0)
    for e in range(n_emb):
        buf = e % 2
        if e + 1 < n_emb:
            issue(e + 1)

        def drain(s, _):
            pltpu.make_async_copy(
                tables.at[:, pl.ds(0, 8 * PICK), :], blocks.at[buf, :, pl.ds(0, 8 * PICK), :], sem.at[buf]).wait()
            return 0

        lax.fori_loop(0, cnt_ref[e], drain, 0)

        def take(b, _):
            r = pl.multiple_of(b * PICK, PICK)
            pick = pick_ref[pl.ds(pl.multiple_of(e * cap + r, PICK), PICK), :]
            for l in range(n_layers):
                rows = blocks[buf, l, pl.ds(pl.multiple_of(r * 8, 8 * PICK), 8 * PICK), :]
                out_ref[e, pl.ds(l * cap + r, PICK), :] = jnp.dot(pick, rows, preferred_element_type=F32).astype(BF)
            return 0

        lax.fori_loop(0, cnt_ref[e], take, 0)

        def rest(b, _):
            r = pl.multiple_of(b * PICK, PICK)
            for l in range(n_layers):
                out_ref[e, pl.ds(l * cap + r, PICK), :] = jnp.zeros((PICK, out_ref.shape[2]), BF)
            return 0

        lax.fori_loop(cnt_ref[e], cap // PICK, rest, 0)


def serve_rows(tables, counts, rows, pick, cap):
    n_layers, _, width = tables.shape
    n_emb = counts.shape[0]
    smem = pl.BlockSpec(memory_space=pltpu.SMEM)
    vmem = pl.BlockSpec(memory_space=pltpu.VMEM)
    return pl.pallas_call(
        functools.partial(serve_kernel, n_layers, cap),
        out_shape=jax.ShapeDtypeStruct((n_emb, n_layers * cap, width), BF),
        in_specs=[smem, smem, vmem, pl.BlockSpec(memory_space=pltpu.HBM)],
        out_specs=vmem,
        scratch_shapes=[
            pltpu.VMEM((2, n_layers, cap * 8, width), BF),
            pltpu.SemaphoreType.DMA((2,)),
        ],
        compiler_params=pltpu.CompilerParams(vmem_limit_bytes=48 << 20),
        cost_estimate=pl.CostEstimate(flops=20_000_000_000, bytes_accessed=30_000_000, transcendentals=0),
        name="serve_rows",
    )(counts, rows, pick, tables)


N_SRC = 16
MAX_ROWS = 17 * BLK


def pull_runs(meta_ref, src, col, dst, sem):
    src_rows = src.shape[0] // N_SRC
    width = dst.shape[1]

    def run(k, _):
        lo, off = meta_ref[k], meta_ref[2 * N_SRC + k]

        def chunk(c, _):
            a = pl.multiple_of(k * src_rows + lo + c * CHUNK, CHUNK)
            b = pl.multiple_of((off + c) * CHUNK, CHUNK)
            pltpu.make_async_copy(src.at[pl.ds(a, CHUNK), col:col + width], dst.at[pl.ds(b, CHUNK), :], sem).start()
            return 0

        return lax.fori_loop(0, meta_ref[N_SRC + k], chunk, 0)

    lax.fori_loop(0, N_SRC, run, 0)


def drain_runs(meta_ref, src, col, dst, sem):
    width = dst.shape[1]

    def one(c, _):
        pltpu.make_async_copy(src.at[pl.ds(0, CHUNK), col:col + width], dst.at[pl.ds(0, CHUNK), :], sem).wait()
        return 0

    lax.fori_loop(0, meta_ref[3 * N_SRC], one, 0)


def n_blocks(meta_ref):
    return lax.div(meta_ref[3 * N_SRC] * CHUNK + BLK - 1, BLK)


def gate_kernel(layer, col, meta_ref, u_hbm, w_ref, out, uc, stage, sem_u, sem_o):
    pull_runs(meta_ref, u_hbm, col, uc, sem_u)
    drain_runs(meta_ref, u_hbm, col, uc, sem_u)
    total = n_blocks(meta_ref)

    def out_copy(b):
        buf = lax.rem(b, 2)
        r = pl.multiple_of(b * BLK, BLK)
        return pltpu.make_async_copy(stage.at[buf], out.at[pl.ds(r, BLK), :], sem_o.at[buf])

    def block(b, _):
        @pl.when(b >= 2)
        def _():
            out_copy(b - 2).wait()

        u = uc[pl.ds(pl.multiple_of(b * BLK, BLK), BLK), :]
        for n in range(4):
            pre = jnp.dot(u, w_ref[layer, :, n * 256:(n + 1) * 256], preferred_element_type=F32)
            stage[lax.rem(b, 2), :, n * 256:(n + 1) * 256] = jax.nn.gelu(pre)
        out_copy(b).start()
        return 0

    lax.fori_loop(0, total, block, 0)
    lax.fori_loop(jnp.maximum(total - 2, 0), total, lambda b, c: (out_copy(b).wait(), c)[1], 0)


def owner_gate(layer, meta, u_all, col, w_gate):
    smem = pl.BlockSpec(memory_space=pltpu.SMEM)
    hbm = pl.BlockSpec(memory_space=pltpu.HBM)
    width = w_gate.shape[2]
    return pl.pallas_call(
        functools.partial(gate_kernel, layer, col),
        out_shape=pltpu.HBM((MAX_ROWS, width), F32),
        in_specs=[smem, hbm, pl.BlockSpec(memory_space=pltpu.VMEM)],
        out_specs=hbm,
        scratch_shapes=[
            pltpu.VMEM((MAX_ROWS, width), BF),
            pltpu.VMEM((2, BLK, width), F32),
            pltpu.SemaphoreType.DMA,
            pltpu.SemaphoreType.DMA((2,)),
        ],
        compiler_params=pltpu.CompilerParams(vmem_limit_bytes=28 << 20),
        cost_estimate=pl.CostEstimate(flops=10_000_000_000, bytes_accessed=30_000_000, transcendentals=0),
    )(meta, u_all, w_gate)


UNROLL = 8


def owner_kernel(layer, col, meta_ref, tile_ref, addr_ref, g_hbm, d_hbm, *rest):
    out, dc, gbuf, prod, acc, sem_d, sem_g, sem_o = rest[-8:]
    n_tiles = tile_ref.shape[0] - 1
    total = n_blocks(meta_ref)

    def g_copy(b):
        buf = lax.rem(b, 2)
        return pltpu.make_async_copy(g_hbm.at[pl.ds(pl.multiple_of(b * BLK, BLK), BLK), :], gbuf.at[buf], sem_g.at[buf])

    g_copy(0).start()
    pull_runs(meta_ref, d_hbm, col, dc, sem_d)
    drain_runs(meta_ref, d_hbm, col, dc, sem_d)

    def block(b, _):
        g_copy(b).wait()

        @pl.when(b + 1 < total)
        def _():
            g_copy(b + 1).start()

        buf = lax.rem(b, 2)
        for t in range(BLK // 16):
            d = dc[pl.ds(pl.multiple_of(b * BLK + t * 16, 16), 16), :].astype(F32)
            val = gbuf[buf, t * 16:(t + 1) * 16, :] * d
            for h in range(2):
                for j in range(8):
                    prod[pl.ds(pl.multiple_of(b * (BLK * 8) + (2 * t + h) * 64 + j * 8, 8), 8), :] = (
                        val[h * 8:(h + 1) * 8, j * 128:(j + 1) * 128])
        return 0

    lax.fori_loop(0, total, block, 0)

    def out_copy(t, buf):
        return pltpu.make_async_copy(
            acc.at[buf].reshape(TILE_ROWS // 8, 8, 8, 128),
            out.at[layer, pl.ds(t * (TILE_ROWS // 8), TILE_ROWS // 8)], sem_o.at[buf])

    def tile(t, _):
        buf = lax.rem(t, 2)

        @pl.when(t >= 2)
        def _():
            out_copy(t - 2, buf).wait()

        def clear(i, _):
            acc[buf, pl.ds(pl.multiple_of(i * 512, 512), 512), :] = jnp.zeros((512, 128), F32)
            return 0

        lax.fori_loop(0, TILE_ROWS * 8 // 512, clear, 0)
        first, last = tile_ref[t], tile_ref[t + 1]

        def one(i, run):
            word = addr_ref[i]
            pa = lax.bitwise_and(word, 0xFFFF)
            ra = lax.bitwise_and(lax.shift_right_logical(word, 16), 0x1FFF)
            fresh = word >= (1 << 29)
            run = jnp.where(fresh, 0.0, run) + prod[pl.ds(pa, 8, stride=8), :]
            acc[buf, pl.ds(ra, 8, stride=8), :] = run
            return run

        def many(i, run):
            for u in range(UNROLL):
                run = one(first + i * UNROLL + u, run)
            return run

        groups = lax.div(last - first, UNROLL)
        run = lax.fori_loop(0, groups, many, jnp.zeros((8, 128), F32))
        lax.fori_loop(first + groups * UNROLL, last, one, run)
        out_copy(t, buf).start()
        return 0

    lax.fori_loop(0, n_tiles, tile, 0)
    out_copy(n_tiles - 2, n_tiles % 2).wait()
    out_copy(n_tiles - 1, (n_tiles - 1) % 2).wait()


def owner_grad(layer, out_prev, out_shape, meta, tiles, addrs, g_rows, d_all, col):
    smem = pl.BlockSpec(memory_space=pltpu.SMEM)
    hbm = pl.BlockSpec(memory_space=pltpu.HBM)
    width = g_rows.shape[1]
    args = [meta, tiles, addrs, g_rows, d_all]
    specs = [smem, smem, smem, hbm, hbm]
    aliases = {}
    if out_prev is not None:
        args.append(out_prev)
        specs.append(hbm)
        aliases = {5: 0}
    return pl.pallas_call(
        functools.partial(owner_kernel, layer, col),
        out_shape=jax.ShapeDtypeStruct(out_shape, F32),
        in_specs=specs,
        out_specs=hbm,
        scratch_shapes=[
            pltpu.VMEM((MAX_ROWS, width), BF),
            pltpu.VMEM((2, BLK, width), F32),
            pltpu.VMEM((MAX_ROWS * 8, 128), F32),
            pltpu.VMEM((2, TILE_ROWS * 8, 128), F32),
            pltpu.SemaphoreType.DMA,
            pltpu.SemaphoreType.DMA((2,)),
            pltpu.SemaphoreType.DMA((2,)),
        ],
        input_output_aliases=aliases,
        compiler_params=pltpu.CompilerParams(vmem_limit_bytes=48 << 20),
        cost_estimate=pl.CostEstimate(flops=40_000_000_000, bytes_accessed=100_000_000, transcendentals=0),
    )(*args)


def solution(mesh):
    n_emb = mesh.shape['emb']
    n_dev = n_emb * mesh.shape['dp']
    tok_spec = P(('dp', 'emb'))
    act_spec = P(('dp', 'emb'), None)
    table_spec = P(None, 'emb', None)
    full_spec = P(None, None, None)
    everyone = ('dp', 'emb')

    def device_body(tok_ids, resid_in, cot_out, tables, w_up, w_down, w_gate, w_proj):
        n_layers, range_rows, width = tables.shape
        n_tok = tok_ids.shape[0]
        cap = min(2 * n_tok // n_emb, 3 * n_tok // 4)
        i_dp, i_emb = lax.axis_index('dp'), lax.axis_index('emb')
        last = n_layers - 1

        def gather(rows):
            return lax.all_gather(rows, everyone, axis=0, tiled=True)

        pos = jnp.arange(n_tok, dtype=jnp.int32)
        before = (tok_ids[None, :] < tok_ids[:, None]) | ((tok_ids[None, :] == tok_ids[:, None]) & (pos[None, :] < pos[:, None]))
        rank = jnp.sum(before.astype(jnp.int32), axis=1)
        perm_mask = rank[None, :] == pos[:, None]
        perm = perm_mask.astype(BF)
        x = jnp.dot(perm, resid_in, preferred_element_type=F32).astype(BF)
        cot = jnp.dot(perm, cot_out, preferred_element_type=F32).astype(BF)
        normed = rms_norm(x.astype(F32)).astype(BF)
        d_mixed = mixed_cot(cot, w_proj[last])
        first_set = jnp.concatenate([normed, d_mixed], axis=1)
        set_a = gather(first_set)

        ids = jnp.sum(jnp.where(perm_mask, tok_ids[None, :], 0), axis=1)
        ids, _ = lax.optimization_barrier((ids, first_set))
        ids_all = lax.all_gather(ids, everyone, axis=0, tiled=True)
        ids_2d = ids_all.reshape(n_dev, n_tok)
        base = i_emb * range_rows

        mine = lax.dynamic_slice(ids_2d, (i_dp * n_emb, 0), (n_emb, n_tok))
        peer_lo = jnp.sum((mine < base).astype(jnp.int32), axis=1)
        peer_hi = jnp.sum((mine < base + range_rows).astype(jnp.int32), axis=1)
        count = peer_hi - peer_lo
        padded = jnp.pad(mine - base, ((0, 0), (0, cap)))
        asked = jax.vmap(lambda r, s: lax.dynamic_slice(r, (s,), (cap,)))(padded, peer_lo)
        slot_pos = jnp.arange(cap, dtype=jnp.int32)
        valid = slot_pos[None, :] < count[:, None]
        asked = jnp.where(valid, asked, 0)
        pick_col = jnp.where(valid, (slot_pos[None, :] % PICK) * 8 + asked % 8, -1).reshape(-1, 1)
        pick8 = (pick_col == jnp.arange(8 * PICK, dtype=jnp.int32)[None, :]).astype(BF)
        served = serve_rows(tables, (count + PICK - 1) // PICK, (asked // 8 * 8).reshape(-1), pick8, cap)
        returned = lax.all_to_all(served, 'emb', 0, 0, tiled=True)
        returned = returned.reshape(n_emb, n_layers, cap, -1)
        owner = ids // range_rows
        first = jnp.sum((owner[None, :] < owner[:, None]).astype(jnp.int32), axis=1)
        slot = owner * cap + pos - first
        pick = (slot[:, None] == jnp.arange(n_emb * cap, dtype=jnp.int32)[None, :]).astype(BF)

        saved, us = [], [normed]
        for l in range(n_layers):
            rows_l = returned[:, l].reshape(n_emb * cap, -1)
            fetched = jnp.dot(pick, rows_l, preferred_element_type=F32).astype(BF)
            x, kept = layer_forward(x, normed, fetched, w_up[l], w_down[l], w_gate[l], w_proj[l])
            saved.append(kept)
            if l < last:
                normed = rms_norm(x.astype(F32)).astype(BF)
                us.append(normed)
        set_b = gather(jnp.concatenate(us[1:], axis=1))
        resid_out = lax.dot_general(perm, x, (((0,), (0,)), ((), ())), preferred_element_type=F32).astype(BF)
        d_sets = [None] * n_layers
        for l in range(last, 0, -1):
            cot = layer_backward(cot, d_mixed, saved[l], w_up[l], w_down[l], w_gate[l])
            d_mixed = mixed_cot(cot, w_proj[l - 1])
            d_sets[l - 1] = (gather(d_mixed), 0)

        n_tiles = range_rows // TILE_ROWS
        lo = jnp.sum((ids_2d < base).astype(jnp.int32), axis=1)
        hi = jnp.sum((ids_2d < base + range_rows).astype(jnp.int32), axis=1)
        lo16 = (lo // CHUNK) * CHUNK
        n_ch = (hi - lo16 + CHUNK - 1) // CHUNK
        tri = jnp.arange(n_dev)[None, :] < jnp.arange(n_dev)[:, None]
        off = jnp.sum(jnp.where(tri, n_ch[None, :], 0), axis=1)
        meta = jnp.concatenate([lo16, n_ch, off, jnp.sum(n_ch)[None]]).astype(jnp.int32)
        place = (off * CHUNK - lo16)[:, None] + pos[None, :]
        local = ids_2d - base
        owned = (local >= 0) & (local < range_rows)
        key = jnp.where(owned, local * (1 << 13) + place, jnp.iinfo(jnp.int32).max)
        key = lax.sort(key.reshape(-1), is_stable=False)[:n_emb * n_dev * cap // 4]
        p, r = key & ((1 << 13) - 1), key >> 13
        fresh = jnp.concatenate([jnp.ones((1,), jnp.bool_), r[1:] != r[:-1]])
        in_tile = r % TILE_ROWS
        addrs = ((p // 8) * 64 + p % 8) | (((in_tile // 8) * 64 + in_tile % 8) << 16) | (fresh.astype(jnp.int32) << 29)
        edges = jnp.arange(n_tiles + 1, dtype=jnp.int32) * TILE_ROWS
        tiles = jnp.sum((r[None, :] < edges[:, None]).astype(jnp.int32), axis=1)

        set_a, _ = lax.optimization_barrier((set_a, d_mixed))
        u_sets = [(set_a, 0)] + [(set_b, i * width) for i in range(n_layers - 1)]
        d_sets[last] = (set_a, width)
        grads = None
        out_shape = (n_layers, range_rows // 8, width // 128, 8, 128)
        gates = [owner_gate(l, meta, *u_sets[l], w_gate) for l in range(n_layers)]
        for l in range(last, -1, -1):
            grads = owner_grad(l, grads, out_shape, meta, tiles, addrs, gates[l], *d_sets[l])
        d_tables = grads.transpose(0, 1, 3, 2, 4).reshape(n_layers, range_rows, width)
        return resid_out, d_tables

    return jax.shard_map(device_body, mesh=mesh, in_specs=(tok_spec, act_spec, act_spec, table_spec, full_spec, full_spec, full_spec, full_spec), out_specs=(act_spec, table_spec), check_vma=False)
```

```python
import functools

import jax
import jax.numpy as jnp
from jax import lax
from jax.experimental import pallas as pl
from jax.experimental.pallas import tpu as pltpu
from jax.sharding import PartitionSpec as P


NORM_EPS = 1e-6
BF = jnp.bfloat16
F32 = jnp.float32

CHUNK = 16
BLK = 256
TILE_ROWS = 1024


def rms_norm(x_f32):
    return x_f32 * lax.rsqrt(jnp.mean(x_f32 * x_f32, axis=-1, keepdims=True) + NORM_EPS)


def share_kernel(n_dp, n_emb, ids_ref, out_ref, local_sem, send_sem, recv_sem):
    n = n_dp * n_emb
    me = lax.axis_index('dp') * n_emb + lax.axis_index('emb')

    def place(o):
        to = lax.rem(me + o, n)
        return (to // n_emb, lax.rem(to, n_emb))

    barrier = pltpu.get_barrier_semaphore()
    for o in range(1, n):
        pl.semaphore_signal(barrier, inc=1, device_id=place(o), device_id_type=pl.DeviceIdType.MESH)
    pl.semaphore_wait(barrier, n - 1)
    sends = [
        pltpu.make_async_remote_copy(
            src_ref=ids_ref, dst_ref=out_ref.at[me], send_sem=send_sem.at[o], recv_sem=recv_sem.at[o],
            device_id=place(o), device_id_type=pl.DeviceIdType.MESH)
        for o in range(1, n)
    ]
    for cp in sends:
        cp.start()
    out_ref[me] = ids_ref[...]
    for cp in sends:
        cp.wait()


def share_ids(ids, n_dp, n_emb):
    n = n_dp * n_emb
    rows = ids.shape[0] // 128
    vmem = pl.BlockSpec(memory_space=pltpu.VMEM)
    out = pl.pallas_call(
        functools.partial(share_kernel, n_dp, n_emb),
        out_shape=jax.ShapeDtypeStruct((n, rows, 128), jnp.int32),
        in_specs=[vmem], out_specs=vmem,
        scratch_shapes=[pltpu.SemaphoreType.DMA, pltpu.SemaphoreType.DMA((n,)), pltpu.SemaphoreType.DMA((n,))],
        compiler_params=pltpu.CompilerParams(collective_id=0, has_side_effects=True),
        name="share_ids",
    )(ids.reshape(rows, 128))
    return out.reshape(-1)


FCH = 512
N_BUF = 3
GELU_C = 0.7978845608028654
GELU_A = 0.044715


def gelu_grad(v):
    t = jnp.tanh(GELU_C * (v + GELU_A * (v * v * v)))
    return 0.5 * (1.0 + t) + (0.5 * GELU_C) * v * (1.0 - t * t) * (1.0 + (3 * GELU_A) * (v * v))


def dot_nt(a, b):
    return lax.dot_general(a, b, (((1,), (1,)), ((), ())), preferred_element_type=F32)


def dot_nn(a, b):
    return jnp.dot(a, b, preferred_element_type=F32)


def stream(layer, w_up, w_down, up_buf, down_buf, sem):
    def copies(c):
        buf = lax.rem(c, N_BUF)
        f = pl.multiple_of(c * FCH, FCH)
        return (pltpu.make_async_copy(w_up.at[layer, :, pl.ds(f, FCH)], up_buf.at[buf], sem.at[0, buf]),
                pltpu.make_async_copy(w_down.at[layer, pl.ds(f, FCH), :], down_buf.at[buf], sem.at[1, buf]))

    return copies


def forward_kernel(layer, keep, x_ref, u_ref, rows_ref, pick_ref, w_up, w_down, w_gate, w_proj, *rest):
    if keep:
        x_out, u_out, up_hbm, gate_hbm, got_out = rest[:5]
        up_buf, down_buf, gate_w, proj_w, acc, up_stage, gate_stage, sem, sem_gp, sem_o = rest[5:]
    else:
        x_out, u_out = rest[:2]
        up_buf, down_buf, gate_w, proj_w, acc, sem, sem_gp = rest[2:]
    n_ch = w_up.shape[2] // FCH
    copies = stream(layer, w_up, w_down, up_buf, down_buf, sem)
    for c in range(N_BUF - 1):
        for cp in copies(c):
            cp.start()
    gate_cp = pltpu.make_async_copy(w_gate.at[layer], gate_w, sem_gp.at[0])
    proj_cp = pltpu.make_async_copy(w_proj.at[layer], proj_w, sem_gp.at[1])
    gate_cp.start()
    proj_cp.start()

    def stage_copy(c):
        buf = lax.rem(c, 2)
        return pltpu.make_async_copy(
            up_stage.at[buf], up_hbm.at[:, pl.ds(pl.multiple_of(c * FCH, FCH), FCH)], sem_o.at[buf])

    acc[...] = x_ref[...].astype(F32)

    def chunk(c, _):
        @pl.when(c + N_BUF - 1 < n_ch)
        def _():
            for cp in copies(c + N_BUF - 1):
                cp.start()

        for cp in copies(c):
            cp.wait()
        if keep:
            @pl.when(c >= 2)
            def _():
                stage_copy(c - 2).wait()

        buf = lax.rem(c, N_BUF)
        hidden = []
        for n in range(FCH // 256):
            pre = dot_nn(u_ref[...], up_buf[buf, :, n * 256:(n + 1) * 256])
            if keep:
                up_stage[lax.rem(c, 2), :, n * 256:(n + 1) * 256] = pre
            hidden.append(jax.nn.gelu(pre).astype(BF))
        hidden = jnp.concatenate(hidden, axis=1)
        for n in range(4):
            acc[:, n * 256:(n + 1) * 256] += dot_nn(hidden, down_buf[buf, :, n * 256:(n + 1) * 256])
        if keep:
            stage_copy(c).start()
        return 0

    lax.fori_loop(0, n_ch, chunk, 0)
    gate_cp.wait()
    proj_cp.wait()
    mixed = []
    for n in range(4):
        cols = slice(n * 256, (n + 1) * 256)
        pre = dot_nn(u_ref[...], gate_w[:, cols])
        got = dot_nn(pick_ref[...], rows_ref[:, cols]).astype(BF)
        if keep:
            gate_stage[:, cols] = pre
            got_out[:, cols] = got
        mixed.append((jax.nn.gelu(pre) * got.astype(F32)).astype(BF))
    mixed = jnp.concatenate(mixed, axis=1)
    if keep:
        gate_out = pltpu.make_async_copy(gate_stage, gate_hbm, sem_o.at[2])
        gate_out.start()
    for n in range(4):
        cols = slice(n * 256, (n + 1) * 256)
        x_out[:, cols] = (acc[:, cols] + dot_nn(mixed, proj_w[:, cols])).astype(BF)
    x_next = x_out[...].astype(F32)
    scale = lax.rsqrt(jnp.mean(x_next * x_next, axis=-1, keepdims=True) + NORM_EPS)
    u_out[...] = (x_next * scale).astype(BF)
    if keep:
        gate_out.wait()
        stage_copy(n_ch - 2).wait()
        stage_copy(n_ch - 1).wait()


def layer_fwd(layer, keep, x, u, rows, pick, w_up, w_down, w_gate, w_proj):
    t, d = x.shape
    f = w_up.shape[2]
    hbm = pl.BlockSpec(memory_space=pltpu.HBM)
    vmem = pl.BlockSpec(memory_space=pltpu.VMEM)
    act = jax.ShapeDtypeStruct((t, d), BF)
    out_shape = [act, act]
    out_specs = [vmem, vmem]
    scratch = [
        pltpu.VMEM((N_BUF, d, FCH), BF), pltpu.VMEM((N_BUF, FCH, d), BF),
        pltpu.VMEM((d, d), BF), pltpu.VMEM((d, d), BF), pltpu.VMEM((t, d), F32),
    ]
    sems = [pltpu.SemaphoreType.DMA((2, N_BUF)), pltpu.SemaphoreType.DMA((2,))]
    if keep:
        out_shape += [pltpu.HBM((t, f), F32), pltpu.HBM((t, d), F32), act]
        out_specs += [hbm, hbm, vmem]
        scratch += [pltpu.VMEM((2, t, FCH), F32), pltpu.VMEM((t, d), F32)]
        sems += [pltpu.SemaphoreType.DMA((3,))]
    return pl.pallas_call(
        functools.partial(forward_kernel, layer, keep),
        out_shape=out_shape, in_specs=[vmem] * 4 + [hbm] * 4, out_specs=out_specs,
        scratch_shapes=scratch + sems,
        compiler_params=pltpu.CompilerParams(vmem_limit_bytes=40 << 20),
        cost_estimate=pl.CostEstimate(flops=11_000_000_000, bytes_accessed=30_000_000, transcendentals=0),
    )(x, u, rows, pick, w_up, w_down, w_gate, w_proj)


def backward_kernel(layer, cot_ref, dm_ref, x_ref, got_ref, up_hbm, gate_hbm, w_up, w_down, w_gate, w_proj,
                    cot_out, dm_out, up_buf, down_buf, pre_buf, gate_w, proj_w, gate_pre, acc, sem, sem_gp):
    n_ch = w_up.shape[2] // FCH
    copies = stream(layer, w_up, w_down, up_buf, down_buf, sem)

    def all_copies(c):
        buf = lax.rem(c, N_BUF)
        pre = pltpu.make_async_copy(
            up_hbm.at[:, pl.ds(pl.multiple_of(c * FCH, FCH), FCH)], pre_buf.at[buf], sem.at[2, buf])
        return copies(c) + (pre,)

    for c in range(N_BUF - 1):
        for cp in all_copies(c):
            cp.start()
    gate_cp = pltpu.make_async_copy(w_gate.at[layer], gate_w, sem_gp.at[0])
    pre_cp = pltpu.make_async_copy(gate_hbm, gate_pre, sem_gp.at[1])
    proj_cp = pltpu.make_async_copy(w_proj.at[layer - 1], proj_w, sem_gp.at[2])
    for cp in (gate_cp, pre_cp, proj_cp):
        cp.start()

    def chunk(c, _):
        @pl.when(c + N_BUF - 1 < n_ch)
        def _():
            for cp in all_copies(c + N_BUF - 1):
                cp.start()

        for cp in all_copies(c):
            cp.wait()
        buf = lax.rem(c, N_BUF)
        d_pre = []
        for n in range(FCH // 256):
            cols = slice(n * 256, (n + 1) * 256)
            d_hidden = dot_nt(cot_ref[...], down_buf[buf, cols, :]).astype(BF).astype(F32)
            d_pre.append((d_hidden * gelu_grad(pre_buf[buf, :, cols])).astype(BF))
        d_pre = jnp.concatenate(d_pre, axis=1)
        for n in range(4):
            cols = slice(n * 256, (n + 1) * 256)
            part = dot_nt(d_pre, up_buf[buf, cols, :])
            acc[:, cols] = part + jnp.where(c == 0, 0.0, acc[:, cols])
        return 0

    lax.fori_loop(0, n_ch, chunk, 0)
    for cp in (gate_cp, pre_cp, proj_cp):
        cp.wait()
    d_pre = []
    for n in range(4):
        cols = slice(n * 256, (n + 1) * 256)
        d_act = dm_ref[:, cols].astype(F32) * got_ref[:, cols].astype(F32)
        d_pre.append((d_act * gelu_grad(gate_pre[:, cols])).astype(BF))
    d_pre = jnp.concatenate(d_pre, axis=1)
    for n in range(4):
        cols = slice(n * 256, (n + 1) * 256)
        both = acc[:, cols].astype(BF) + dot_nt(d_pre, gate_w[cols, :]).astype(BF)
        acc[:, cols] = both.astype(F32)
    x = x_ref[...].astype(F32)
    dy = acc[...]
    r = lax.rsqrt(jnp.mean(x * x, axis=-1, keepdims=True) + NORM_EPS)
    proj = jnp.mean(x * dy, axis=-1, keepdims=True)
    cot = (cot_ref[...].astype(F32) + (dy * r - x * (r * r * r * proj))).astype(BF)
    cot_out[...] = cot
    for n in range(4):
        cols = slice(n * 256, (n + 1) * 256)
        dm_out[:, cols] = dot_nt(cot, proj_w[cols, :]).astype(BF)


def layer_bwd(layer, cot, d_mixed, x, got, up_pre, gate_pre, w_up, w_down, w_gate, w_proj):
    t, d = x.shape
    hbm = pl.BlockSpec(memory_space=pltpu.HBM)
    vmem = pl.BlockSpec(memory_space=pltpu.VMEM)
    act = jax.ShapeDtypeStruct((t, d), BF)
    return pl.pallas_call(
        functools.partial(backward_kernel, layer),
        out_shape=[act, act], in_specs=[vmem] * 4 + [hbm] * 6, out_specs=[vmem, vmem],
        scratch_shapes=[
            pltpu.VMEM((N_BUF, d, FCH), BF), pltpu.VMEM((N_BUF, FCH, d), BF), pltpu.VMEM((N_BUF, t, FCH), F32),
            pltpu.VMEM((d, d), BF), pltpu.VMEM((d, d), BF), pltpu.VMEM((t, d), F32), pltpu.VMEM((t, d), F32),
            pltpu.SemaphoreType.DMA((3, N_BUF)), pltpu.SemaphoreType.DMA((3,)),
        ],
        compiler_params=pltpu.CompilerParams(vmem_limit_bytes=40 << 20),
        cost_estimate=pl.CostEstimate(flops=11_000_000_000, bytes_accessed=40_000_000, transcendentals=0),
    )(cot, d_mixed, x, got, up_pre, gate_pre, w_up, w_down, w_gate, w_proj)


PICK = 32


def serve_kernel(n_layers, cap, cnt_ref, start_ref, ids_ref, pick_ref, tables, *rest):
    outs, (blocks, sem) = rest[:n_layers], rest[n_layers:]
    n_emb = outs[0].shape[0]
    range_rows = tables.shape[1]

    def issue(e):
        def body(s, _):
            row = lax.rem(ids_ref[start_ref[e] + s], range_rows)
            row = pl.multiple_of(lax.div(row, 8) * 8, 8)
            slot = pl.multiple_of(s * 8, 8)
            pltpu.make_async_copy(
                tables.at[:, pl.ds(row, 8), :], blocks.at[e % 2, :, pl.ds(slot, 8), :], sem.at[e % 2]).start()
            return 0

        lax.fori_loop(0, cnt_ref[e] * PICK, body, 0)

    issue(0)
    for e in range(n_emb):
        buf = e % 2
        if e + 1 < n_emb:
            issue(e + 1)

        def drain(s, _):
            pltpu.make_async_copy(
                tables.at[:, pl.ds(0, 8 * PICK), :], blocks.at[buf, :, pl.ds(0, 8 * PICK), :], sem.at[buf]).wait()
            return 0

        lax.fori_loop(0, cnt_ref[e], drain, 0)

        def take(b, _):
            r = pl.multiple_of(b * PICK, PICK)
            pick = pick_ref[pl.ds(pl.multiple_of(e * cap + r, PICK), PICK), :]
            for l in range(n_layers):
                rows = blocks[buf, l, pl.ds(pl.multiple_of(r * 8, 8 * PICK), 8 * PICK), :]
                outs[l][e, pl.ds(r, PICK), :] = jnp.dot(pick, rows, preferred_element_type=F32).astype(BF)
            return 0

        lax.fori_loop(0, cnt_ref[e], take, 0)

        def rest(b, _):
            r = pl.multiple_of(b * PICK, PICK)
            for l in range(n_layers):
                outs[l][e, pl.ds(r, PICK), :] = jnp.zeros((PICK, outs[l].shape[2]), BF)
            return 0

        lax.fori_loop(cnt_ref[e], cap // PICK, rest, 0)


def serve_rows(tables, counts, starts, ids, pick, cap):
    n_layers, _, width = tables.shape
    n_emb = counts.shape[0]
    smem = pl.BlockSpec(memory_space=pltpu.SMEM)
    vmem = pl.BlockSpec(memory_space=pltpu.VMEM)
    return pl.pallas_call(
        functools.partial(serve_kernel, n_layers, cap),
        out_shape=[jax.ShapeDtypeStruct((n_emb, cap, width), BF)] * n_layers,
        in_specs=[smem, smem, smem, vmem, pl.BlockSpec(memory_space=pltpu.HBM)],
        out_specs=[vmem] * n_layers,
        scratch_shapes=[
            pltpu.VMEM((2, n_layers, cap * 8, width), BF),
            pltpu.SemaphoreType.DMA((2,)),
        ],
        compiler_params=pltpu.CompilerParams(vmem_limit_bytes=48 << 20),
        cost_estimate=pl.CostEstimate(flops=20_000_000_000, bytes_accessed=30_000_000, transcendentals=0),
        name="serve_rows",
    )(counts, starts, ids, pick, tables)


N_SRC = 16
MAX_ROWS = 17 * BLK


def pull_runs(meta_ref, src, col, dst, sem):
    src_rows = src.shape[0] // N_SRC
    width = dst.shape[1]

    def run(k, _):
        lo, off = meta_ref[k], meta_ref[2 * N_SRC + k]

        def chunk(c, _):
            a = pl.multiple_of(k * src_rows + lo + c * CHUNK, CHUNK)
            b = pl.multiple_of((off + c) * CHUNK, CHUNK)
            pltpu.make_async_copy(src.at[pl.ds(a, CHUNK), col:col + width], dst.at[pl.ds(b, CHUNK), :], sem).start()
            return 0

        return lax.fori_loop(0, meta_ref[N_SRC + k], chunk, 0)

    lax.fori_loop(0, N_SRC, run, 0)


def drain_runs(meta_ref, src, col, dst, sem):
    width = dst.shape[1]

    def one(c, _):
        pltpu.make_async_copy(src.at[pl.ds(0, CHUNK), col:col + width], dst.at[pl.ds(0, CHUNK), :], sem).wait()
        return 0

    lax.fori_loop(0, meta_ref[3 * N_SRC], one, 0)


def n_blocks(meta_ref):
    return lax.div(meta_ref[3 * N_SRC] * CHUNK + BLK - 1, BLK)


def gate_kernel(layer, col, meta_ref, u_hbm, w_ref, out, uc, stage, sem_u, sem_o):
    pull_runs(meta_ref, u_hbm, col, uc, sem_u)
    drain_runs(meta_ref, u_hbm, col, uc, sem_u)
    total = n_blocks(meta_ref)

    def out_copy(b):
        buf = lax.rem(b, 2)
        return pltpu.make_async_copy(stage.at[buf], out.at[pl.ds(b * (BLK // 8), BLK // 8)], sem_o.at[buf])

    def block(b, _):
        @pl.when(b >= 2)
        def _():
            out_copy(b - 2).wait()

        u = uc[pl.ds(pl.multiple_of(b * BLK, BLK), BLK), :]
        for n in range(4):
            pre = jnp.dot(u, w_ref[layer, :, n * 256:(n + 1) * 256], preferred_element_type=F32)
            act = jax.nn.gelu(pre)
            for j in range(2):
                stage[lax.rem(b, 2), :, n * 2 + j] = act[:, j * 128:(j + 1) * 128].reshape(BLK // 8, 8, 128)
        out_copy(b).start()
        return 0

    lax.fori_loop(0, total, block, 0)
    lax.fori_loop(jnp.maximum(total - 2, 0), total, lambda b, c: (out_copy(b).wait(), c)[1], 0)


def owner_gate(layer, meta, u_all, col, w_gate):
    smem = pl.BlockSpec(memory_space=pltpu.SMEM)
    hbm = pl.BlockSpec(memory_space=pltpu.HBM)
    width = w_gate.shape[2]
    return pl.pallas_call(
        functools.partial(gate_kernel, layer, col),
        out_shape=pltpu.HBM((MAX_ROWS // 8, width // 128, 8, 128), F32),
        in_specs=[smem, hbm, pl.BlockSpec(memory_space=pltpu.VMEM)],
        out_specs=hbm,
        scratch_shapes=[
            pltpu.VMEM((MAX_ROWS, width), BF),
            pltpu.VMEM((2, BLK // 8, width // 128, 8, 128), F32),
            pltpu.SemaphoreType.DMA,
            pltpu.SemaphoreType.DMA((2,)),
        ],
        compiler_params=pltpu.CompilerParams(vmem_limit_bytes=28 << 20),
        cost_estimate=pl.CostEstimate(flops=10_000_000_000, bytes_accessed=30_000_000, transcendentals=0),
    )(meta, u_all, w_gate)


UNROLL = 8


def owner_kernel(layer, col, meta_ref, tile_ref, addr_ref, g_hbm, d_hbm, *rest):
    out, dc, prod, acc, sem_d, sem_g, sem_o = rest[-7:]
    n_tiles = tile_ref.shape[0] - 1
    total = n_blocks(meta_ref)

    def g_copy(b):
        n = BLK // 8
        return pltpu.make_async_copy(
            g_hbm.at[pl.ds(b * n, n)], prod.reshape(MAX_ROWS // 8, 8, 8, 128).at[pl.ds(b * n, n)], sem_g.at[b])

    pull_runs(meta_ref, d_hbm, col, dc, sem_d)
    lax.fori_loop(0, total, lambda b, c: (g_copy(b).start(), c)[1], 0)

    def clear(buf):
        def some(i, _):
            acc[buf, pl.ds(pl.multiple_of(i * 512, 512), 512), :] = jnp.zeros((512, 128), F32)
            return 0

        lax.fori_loop(0, TILE_ROWS * 8 // 512, some, 0)

    clear(0)
    clear(1)
    drain_runs(meta_ref, d_hbm, col, dc, sem_d)

    def block(b, _):
        g_copy(b).wait()
        for t in range(BLK // 16):
            d = dc[pl.ds(pl.multiple_of(b * BLK + t * 16, 16), 16), :].astype(F32)
            for h in range(2):
                for j in range(8):
                    at = pl.ds(pl.multiple_of(b * (BLK * 8) + (2 * t + h) * 64 + j * 8, 8), 8)
                    prod[at, :] = prod[at, :] * d[h * 8:(h + 1) * 8, j * 128:(j + 1) * 128]
        return 0

    lax.fori_loop(0, total, block, 0)

    def out_copy(t, buf):
        return pltpu.make_async_copy(
            acc.at[buf].reshape(TILE_ROWS // 8, 8, 8, 128),
            out.at[layer, pl.ds(t * (TILE_ROWS // 8), TILE_ROWS // 8)], sem_o.at[buf])

    def tile(t, _):
        buf = lax.rem(t, 2)

        @pl.when(t >= 2)
        def _():
            out_copy(t - 2, buf).wait()
            clear(buf)

        first, last = tile_ref[t], tile_ref[t + 1]

        def one(i, run):
            word = addr_ref[i]
            pa = lax.bitwise_and(word, 0xFFFF)
            ra = lax.bitwise_and(lax.shift_right_logical(word, 16), 0x1FFF)
            fresh = word >= (1 << 29)
            run = jnp.where(fresh, 0.0, run) + prod[pl.ds(pa, 8, stride=8), :]
            acc[buf, pl.ds(ra, 8, stride=8), :] = run
            return run

        def many(i, run):
            for u in range(UNROLL):
                run = one(first + i * UNROLL + u, run)
            return run

        groups = lax.div(last - first, UNROLL)
        run = lax.fori_loop(0, groups, many, jnp.zeros((8, 128), F32))
        lax.fori_loop(first + groups * UNROLL, last, one, run)
        out_copy(t, buf).start()
        return 0

    lax.fori_loop(0, n_tiles, tile, 0)
    out_copy(n_tiles - 2, n_tiles % 2).wait()
    out_copy(n_tiles - 1, (n_tiles - 1) % 2).wait()


def owner_grad(layer, out_prev, out_shape, meta, tiles, addrs, g_rows, d_all, col):
    smem = pl.BlockSpec(memory_space=pltpu.SMEM)
    hbm = pl.BlockSpec(memory_space=pltpu.HBM)
    width = g_rows.shape[1] * 128
    args = [meta, tiles, addrs, g_rows, d_all]
    specs = [smem, smem, smem, hbm, hbm]
    aliases = {}
    if out_prev is not None:
        args.append(out_prev)
        specs.append(hbm)
        aliases = {5: 0}
    return pl.pallas_call(
        functools.partial(owner_kernel, layer, col),
        out_shape=jax.ShapeDtypeStruct(out_shape, F32),
        in_specs=specs,
        out_specs=hbm,
        scratch_shapes=[
            pltpu.VMEM((MAX_ROWS, width), BF),
            pltpu.VMEM((MAX_ROWS * 8, 128), F32),
            pltpu.VMEM((2, TILE_ROWS * 8, 128), F32),
            pltpu.SemaphoreType.DMA,
            pltpu.SemaphoreType.DMA((MAX_ROWS // BLK,)),
            pltpu.SemaphoreType.DMA((2,)),
        ],
        input_output_aliases=aliases,
        compiler_params=pltpu.CompilerParams(vmem_limit_bytes=48 << 20),
        cost_estimate=pl.CostEstimate(flops=40_000_000_000, bytes_accessed=100_000_000, transcendentals=0),
    )(*args)


def solution(mesh):
    n_emb = mesh.shape['emb']
    n_dev = n_emb * mesh.shape['dp']
    tok_spec = P(('dp', 'emb'))
    act_spec = P(('dp', 'emb'), None)
    table_spec = P(None, 'emb', None)
    full_spec = P(None, None, None)
    everyone = ('dp', 'emb')

    def device_body(tok_ids, resid_in, cot_out, tables, w_up, w_down, w_gate, w_proj):
        n_layers, range_rows, width = tables.shape
        n_dp = n_dev // n_emb
        n_tok = tok_ids.shape[0]
        cap = min(2 * n_tok // n_emb, 3 * n_tok // 4)
        i_dp, i_emb = lax.axis_index('dp'), lax.axis_index('emb')
        last = n_layers - 1

        def gather(rows):
            return lax.all_gather(rows, everyone, axis=0, tiled=True)

        pos = jnp.arange(n_tok, dtype=jnp.int32)
        before = (tok_ids[None, :] < tok_ids[:, None]) | ((tok_ids[None, :] == tok_ids[:, None]) & (pos[None, :] < pos[:, None]))
        rank = jnp.sum(before.astype(jnp.int32), axis=1)
        perm_mask = rank[None, :] == pos[:, None]
        perm = perm_mask.astype(BF)
        x = jnp.dot(perm, resid_in, preferred_element_type=F32).astype(BF)
        cot = jnp.dot(perm, cot_out, preferred_element_type=F32).astype(BF)
        normed = rms_norm(x.astype(F32)).astype(BF)
        d_mixed = lax.dot_general(cot, w_proj[last], (((1,), (1,)), ((), ())), preferred_element_type=F32).astype(BF)
        first_set = jnp.concatenate([normed, d_mixed], axis=1)
        set_a = gather(first_set)

        ids = jnp.sum(jnp.where(perm_mask, tok_ids[None, :], 0), axis=1)
        ids, _ = lax.optimization_barrier((ids, first_set))
        ids_all = share_ids(ids, n_dp, n_emb)
        ids_2d = ids_all.reshape(n_dev, n_tok)
        base = i_emb * range_rows

        mine = lax.dynamic_slice(ids_2d, (i_dp * n_emb, 0), (n_emb, n_tok))
        peer_lo = jnp.sum((mine < base).astype(jnp.int32), axis=1)
        count = jnp.sum((mine < base + range_rows).astype(jnp.int32), axis=1) - peer_lo
        slot_pos = jnp.arange(cap, dtype=jnp.int32)
        at = pos[None, None, :] == (peer_lo[:, None] + slot_pos[None, :])[:, :, None]
        low = jnp.sum(jnp.where(at, mine[:, None, :] % 8, 0), axis=2)
        pick_col = jnp.where(slot_pos[None, :] < count[:, None], (slot_pos[None, :] % PICK) * 8 + low, -1)
        pick8 = (pick_col.reshape(-1, 1) == jnp.arange(8 * PICK, dtype=jnp.int32)[None, :]).astype(BF)
        starts = peer_lo + (i_dp * n_emb + jnp.arange(n_emb, dtype=jnp.int32)) * n_tok
        served = serve_rows(tables, (count + PICK - 1) // PICK, starts, jnp.pad(ids_all, (0, PICK)), pick8, cap)
        returned = [lax.all_to_all(rows, 'emb', 0, 0, tiled=True).reshape(n_emb * cap, width) for rows in served]
        owner = ids // range_rows
        first = jnp.sum((owner[None, :] < owner[:, None]).astype(jnp.int32), axis=1)
        slot = owner * cap + pos - first
        pick = (slot[:, None] == jnp.arange(n_emb * cap, dtype=jnp.int32)[None, :]).astype(BF)

        weights = (w_up, w_down, w_gate, w_proj)
        saved, us = [], [normed]
        for l in range(n_layers):
            x_in = x
            x, u_next, *kept = layer_fwd(l, l > 0, x, us[-1], returned[l], pick, *weights)
            saved.append((x_in, *kept))
            us.append(u_next)
        set_b = gather(jnp.concatenate(us[1:n_layers], axis=1))
        resid_out = lax.dot_general(perm, x, (((0,), (0,)), ((), ())), preferred_element_type=F32).astype(BF)
        d_sets = [None] * n_layers
        for l in range(last, 0, -1):
            x_in, up_pre, gate_pre, got = saved[l]
            cot, d_mixed = layer_bwd(l, cot, d_mixed, x_in, got, up_pre, gate_pre, *weights)
            d_sets[l - 1] = (gather(d_mixed), 0)

        n_tiles = range_rows // TILE_ROWS
        lo = jnp.sum((ids_2d < base).astype(jnp.int32), axis=1)
        hi = jnp.sum((ids_2d < base + range_rows).astype(jnp.int32), axis=1)
        lo16 = (lo // CHUNK) * CHUNK
        n_ch = (hi - lo16 + CHUNK - 1) // CHUNK
        tri = jnp.arange(n_dev)[None, :] < jnp.arange(n_dev)[:, None]
        off = jnp.sum(jnp.where(tri, n_ch[None, :], 0), axis=1)
        meta = jnp.concatenate([lo16, n_ch, off, jnp.sum(n_ch)[None]]).astype(jnp.int32)
        place = (off * CHUNK - lo16)[:, None] + pos[None, :]
        local = ids_2d - base
        owned = (local >= 0) & (local < range_rows)
        key = jnp.where(owned, local * (1 << 13) + place, jnp.iinfo(jnp.int32).max)
        key = lax.sort(key.reshape(-1), is_stable=False)[:n_emb * n_dev * cap // 4]
        p, r = key & ((1 << 13) - 1), key >> 13
        fresh = jnp.concatenate([jnp.ones((1,), jnp.bool_), r[1:] != r[:-1]])
        in_tile = r % TILE_ROWS
        addrs = ((p // 8) * 64 + p % 8) | (((in_tile // 8) * 64 + in_tile % 8) << 16) | (fresh.astype(jnp.int32) << 29)
        edges = jnp.arange(n_tiles + 1, dtype=jnp.int32) * TILE_ROWS
        tiles = jnp.sum((r[None, :] < edges[:, None]).astype(jnp.int32), axis=1)

        set_a, _ = lax.optimization_barrier((set_a, d_mixed))
        u_sets = [(set_a, 0)] + [(set_b, i * width) for i in range(n_layers - 1)]
        d_sets[last] = (set_a, width)
        grads = None
        out_shape = (n_layers, range_rows // 8, width // 128, 8, 128)
        gates = [owner_gate(l, meta, *u_sets[l], w_gate) for l in range(n_layers)]
        for l in range(last, -1, -1):
            grads = owner_grad(l, grads, out_shape, meta, tiles, addrs, gates[l], *d_sets[l])
        d_tables = grads.transpose(0, 1, 3, 2, 4).reshape(n_layers, range_rows, width)
        return resid_out, d_tables

    return jax.shard_map(device_body, mesh=mesh, in_specs=(tok_spec, act_spec, act_spec, table_spec, full_spec, full_spec, full_spec, full_spec), out_specs=(act_spec, table_spec), check_vma=False)
```

```python
import functools

import jax
import jax.numpy as jnp
from jax import lax
from jax.experimental import pallas as pl
from jax.experimental.pallas import tpu as pltpu
from jax.sharding import PartitionSpec as P


NORM_EPS = 1e-6
BF = jnp.bfloat16
F32 = jnp.float32

CHUNK = 16
BLK = 256
TILE_ROWS = 1024


def in_hbm(*arrays):
    return [pltpu.with_memory_space_constraint(a, pltpu.HBM) for a in arrays]


def rms_norm(x_f32):
    return x_f32 * lax.rsqrt(jnp.mean(x_f32 * x_f32, axis=-1, keepdims=True) + NORM_EPS)


def share_kernel(n_dp, n_emb, ids_ref, out_ref, local_sem, send_sem, recv_sem):
    n = n_dp * n_emb
    me = lax.axis_index('dp') * n_emb + lax.axis_index('emb')

    def place(o):
        to = lax.rem(me + o, n)
        return (to // n_emb, lax.rem(to, n_emb))

    barrier = pltpu.get_barrier_semaphore()
    for o in range(1, n):
        pl.semaphore_signal(barrier, inc=1, device_id=place(o), device_id_type=pl.DeviceIdType.MESH)
    pl.semaphore_wait(barrier, n - 1)
    sends = [
        pltpu.make_async_remote_copy(
            src_ref=ids_ref, dst_ref=out_ref.at[me], send_sem=send_sem.at[o], recv_sem=recv_sem.at[o],
            device_id=place(o), device_id_type=pl.DeviceIdType.MESH)
        for o in range(1, n)
    ]
    for cp in sends:
        cp.start()
    out_ref[me] = ids_ref[...]
    for cp in sends:
        cp.wait()


def share_ids(ids, n_dp, n_emb):
    n = n_dp * n_emb
    rows = ids.shape[0] // 128
    vmem = pl.BlockSpec(memory_space=pltpu.VMEM)
    out = pl.pallas_call(
        functools.partial(share_kernel, n_dp, n_emb),
        out_shape=jax.ShapeDtypeStruct((n, rows, 128), jnp.int32),
        in_specs=[vmem], out_specs=vmem,
        scratch_shapes=[pltpu.SemaphoreType.DMA, pltpu.SemaphoreType.DMA((n,)), pltpu.SemaphoreType.DMA((n,))],
        compiler_params=pltpu.CompilerParams(collective_id=0, has_side_effects=True),
        name="share_ids",
    )(ids.reshape(rows, 128))
    return out.reshape(-1)


FCH = 512
N_BUF = 3
GELU_C = 0.7978845608028654
GELU_A = 0.044715


def gelu_grad(v):
    t = jnp.tanh(GELU_C * (v + GELU_A * (v * v * v)))
    return 0.5 * (1.0 + t) + (0.5 * GELU_C) * v * (1.0 - t * t) * (1.0 + (3 * GELU_A) * (v * v))


def dot_nt(a, b):
    return lax.dot_general(a, b, (((1,), (1,)), ((), ())), preferred_element_type=F32)


def dot_nn(a, b):
    return jnp.dot(a, b, preferred_element_type=F32)


def stream(layer, w_up, w_down, up_buf, down_buf, sem):
    def copies(c):
        buf = lax.rem(c, N_BUF)
        f = pl.multiple_of(c * FCH, FCH)
        return (pltpu.make_async_copy(w_up.at[layer, :, pl.ds(f, FCH)], up_buf.at[buf], sem.at[0, buf]),
                pltpu.make_async_copy(w_down.at[layer, pl.ds(f, FCH), :], down_buf.at[buf], sem.at[1, buf]))

    return copies


def forward_kernel(layer, keep, x_ref, u_ref, r0_ref, r1_ref, r2_ref, r3_ref, pick_ref, w_up, w_down, w_gate, w_proj, *rest):
    if keep:
        x_out, u_out, up_hbm, gate_hbm, got_out = rest[:5]
        up_buf, down_buf, gate_w, proj_w, acc, up_stage, gate_stage, sem, sem_gp, sem_o = rest[5:]
    else:
        x_out, u_out = rest[:2]
        up_buf, down_buf, gate_w, proj_w, acc, sem, sem_gp = rest[2:]
    n_ch = w_up.shape[2] // FCH
    copies = stream(layer, w_up, w_down, up_buf, down_buf, sem)
    for c in range(N_BUF - 1):
        for cp in copies(c):
            cp.start()
    gate_cp = pltpu.make_async_copy(w_gate.at[layer], gate_w, sem_gp.at[0])
    proj_cp = pltpu.make_async_copy(w_proj.at[layer], proj_w, sem_gp.at[1])
    gate_cp.start()
    proj_cp.start()

    def stage_copy(c):
        buf = lax.rem(c, 2)
        return pltpu.make_async_copy(
            up_stage.at[buf], up_hbm.at[:, pl.ds(pl.multiple_of(c * FCH, FCH), FCH)], sem_o.at[buf])

    acc[...] = x_ref[...].astype(F32)

    def chunk(c, _):
        @pl.when(c + N_BUF - 1 < n_ch)
        def _():
            for cp in copies(c + N_BUF - 1):
                cp.start()

        for cp in copies(c):
            cp.wait()
        if keep:
            @pl.when(c >= 2)
            def _():
                stage_copy(c - 2).wait()

        buf = lax.rem(c, N_BUF)
        hidden = []
        for n in range(FCH // 256):
            pre = dot_nn(u_ref[...], up_buf[buf, :, n * 256:(n + 1) * 256])
            if keep:
                up_stage[lax.rem(c, 2), :, n * 256:(n + 1) * 256] = pre
            hidden.append(jax.nn.gelu(pre).astype(BF))
        hidden = jnp.concatenate(hidden, axis=1)
        for n in range(4):
            acc[:, n * 256:(n + 1) * 256] += dot_nn(hidden, down_buf[buf, :, n * 256:(n + 1) * 256])
        if keep:
            stage_copy(c).start()
        return 0

    lax.fori_loop(0, n_ch, chunk, 0)
    gate_cp.wait()
    proj_cp.wait()
    mixed = []
    for n in range(4):
        cols = slice(n * 256, (n + 1) * 256)
        pre = dot_nn(u_ref[...], gate_w[:, cols])
        cap = r0_ref.shape[0]
        got = sum(dot_nn(pick_ref[:, f * cap:(f + 1) * cap], r[:, cols])
                  for f, r in enumerate((r0_ref, r1_ref, r2_ref, r3_ref))).astype(BF)
        if keep:
            gate_stage[:, cols] = pre
            got_out[:, cols] = got
        mixed.append((jax.nn.gelu(pre) * got.astype(F32)).astype(BF))
    mixed = jnp.concatenate(mixed, axis=1)
    if keep:
        gate_out = pltpu.make_async_copy(gate_stage, gate_hbm, sem_o.at[2])
        gate_out.start()
    for n in range(4):
        cols = slice(n * 256, (n + 1) * 256)
        x_out[:, cols] = (acc[:, cols] + dot_nn(mixed, proj_w[:, cols])).astype(BF)
    x_next = x_out[...].astype(F32)
    scale = lax.rsqrt(jnp.mean(x_next * x_next, axis=-1, keepdims=True) + NORM_EPS)
    u_out[...] = (x_next * scale).astype(BF)
    if keep:
        gate_out.wait()
        stage_copy(n_ch - 2).wait()
        stage_copy(n_ch - 1).wait()


def layer_fwd(layer, keep, x, u, rows, pick, w_up, w_down, w_gate, w_proj):
    t, d = x.shape
    f = w_up.shape[2]
    hbm = pl.BlockSpec(memory_space=pltpu.HBM)
    vmem = pl.BlockSpec(memory_space=pltpu.VMEM)
    act = jax.ShapeDtypeStruct((t, d), BF)
    out_shape = [act, act]
    out_specs = [vmem, vmem]
    scratch = [
        pltpu.VMEM((N_BUF, d, FCH), BF), pltpu.VMEM((N_BUF, FCH, d), BF),
        pltpu.VMEM((d, d), BF), pltpu.VMEM((d, d), BF), pltpu.VMEM((t, d), F32),
    ]
    sems = [pltpu.SemaphoreType.DMA((2, N_BUF)), pltpu.SemaphoreType.DMA((2,))]
    if keep:
        out_shape += [pltpu.HBM((t, f), F32), pltpu.HBM((t, d), F32), act]
        out_specs += [hbm, hbm, vmem]
        scratch += [pltpu.VMEM((2, t, FCH), F32), pltpu.VMEM((t, d), F32)]
        sems += [pltpu.SemaphoreType.DMA((3,))]
    return pl.pallas_call(
        functools.partial(forward_kernel, layer, keep),
        out_shape=out_shape, in_specs=[vmem] * 7 + [hbm] * 4, out_specs=out_specs,
        scratch_shapes=scratch + sems,
        compiler_params=pltpu.CompilerParams(vmem_limit_bytes=40 << 20),
        cost_estimate=pl.CostEstimate(flops=11_000_000_000, bytes_accessed=30_000_000, transcendentals=0),
    )(x, u, *rows, pick, *in_hbm(w_up, w_down, w_gate, w_proj))


def backward_kernel(layer, cot_ref, dm_ref, x_ref, got_ref, up_hbm, gate_hbm, w_up, w_down, w_gate, w_proj,
                    cot_out, dm_out, up_buf, down_buf, pre_buf, gate_w, proj_w, gate_pre, acc, sem, sem_gp):
    n_ch = w_up.shape[2] // FCH
    copies = stream(layer, w_up, w_down, up_buf, down_buf, sem)

    def all_copies(c):
        buf = lax.rem(c, N_BUF)
        pre = pltpu.make_async_copy(
            up_hbm.at[:, pl.ds(pl.multiple_of(c * FCH, FCH), FCH)], pre_buf.at[buf], sem.at[2, buf])
        return copies(c) + (pre,)

    for c in range(N_BUF - 1):
        for cp in all_copies(c):
            cp.start()
    gate_cp = pltpu.make_async_copy(w_gate.at[layer], gate_w, sem_gp.at[0])
    pre_cp = pltpu.make_async_copy(gate_hbm, gate_pre, sem_gp.at[1])
    proj_cp = pltpu.make_async_copy(w_proj.at[layer - 1], proj_w, sem_gp.at[2])
    for cp in (gate_cp, pre_cp, proj_cp):
        cp.start()

    def chunk(c, _):
        @pl.when(c + N_BUF - 1 < n_ch)
        def _():
            for cp in all_copies(c + N_BUF - 1):
                cp.start()

        for cp in all_copies(c):
            cp.wait()
        buf = lax.rem(c, N_BUF)
        d_pre = []
        for n in range(FCH // 256):
            cols = slice(n * 256, (n + 1) * 256)
            d_hidden = dot_nt(cot_ref[...], down_buf[buf, cols, :]).astype(BF).astype(F32)
            d_pre.append((d_hidden * gelu_grad(pre_buf[buf, :, cols])).astype(BF))
        d_pre = jnp.concatenate(d_pre, axis=1)
        for n in range(4):
            cols = slice(n * 256, (n + 1) * 256)
            part = dot_nt(d_pre, up_buf[buf, cols, :])
            acc[:, cols] = part + jnp.where(c == 0, 0.0, acc[:, cols])
        return 0

    lax.fori_loop(0, n_ch, chunk, 0)
    for cp in (gate_cp, pre_cp, proj_cp):
        cp.wait()
    d_pre = []
    for n in range(4):
        cols = slice(n * 256, (n + 1) * 256)
        d_act = dm_ref[:, cols].astype(F32) * got_ref[:, cols].astype(F32)
        d_pre.append((d_act * gelu_grad(gate_pre[:, cols])).astype(BF))
    d_pre = jnp.concatenate(d_pre, axis=1)
    for n in range(4):
        cols = slice(n * 256, (n + 1) * 256)
        both = acc[:, cols].astype(BF) + dot_nt(d_pre, gate_w[cols, :]).astype(BF)
        acc[:, cols] = both.astype(F32)
    x = x_ref[...].astype(F32)
    dy = acc[...]
    r = lax.rsqrt(jnp.mean(x * x, axis=-1, keepdims=True) + NORM_EPS)
    proj = jnp.mean(x * dy, axis=-1, keepdims=True)
    cot = (cot_ref[...].astype(F32) + (dy * r - x * (r * r * r * proj))).astype(BF)
    cot_out[...] = cot
    for n in range(4):
        cols = slice(n * 256, (n + 1) * 256)
        dm_out[:, cols] = dot_nt(cot, proj_w[cols, :]).astype(BF)


def layer_bwd(layer, cot, d_mixed, x, got, up_pre, gate_pre, w_up, w_down, w_gate, w_proj):
    t, d = x.shape
    hbm = pl.BlockSpec(memory_space=pltpu.HBM)
    vmem = pl.BlockSpec(memory_space=pltpu.VMEM)
    act = jax.ShapeDtypeStruct((t, d), BF)
    return pl.pallas_call(
        functools.partial(backward_kernel, layer),
        out_shape=[act, act], in_specs=[vmem] * 4 + [hbm] * 6, out_specs=[vmem, vmem],
        scratch_shapes=[
            pltpu.VMEM((N_BUF, d, FCH), BF), pltpu.VMEM((N_BUF, FCH, d), BF), pltpu.VMEM((N_BUF, t, FCH), F32),
            pltpu.VMEM((d, d), BF), pltpu.VMEM((d, d), BF), pltpu.VMEM((t, d), F32), pltpu.VMEM((t, d), F32),
            pltpu.SemaphoreType.DMA((3, N_BUF)), pltpu.SemaphoreType.DMA((3,)),
        ],
        compiler_params=pltpu.CompilerParams(vmem_limit_bytes=40 << 20),
        cost_estimate=pl.CostEstimate(flops=11_000_000_000, bytes_accessed=40_000_000, transcendentals=0),
    )(cot, d_mixed, x, got, *in_hbm(up_pre, gate_pre, w_up, w_down, w_gate, w_proj))


PICK = 32


def serve_kernel(n_layers, cap, cnt_ref, start_ref, ids_ref, pick_ref, tables, *rest):
    blocks, sem = rest[-2:]
    n_emb = len(rest[:-2]) // n_layers
    range_rows = tables.shape[1]

    def issue(e):
        def body(s, _):
            row = lax.rem(ids_ref[start_ref[e] + s], range_rows)
            row = pl.multiple_of(lax.div(row, 8) * 8, 8)
            slot = pl.multiple_of(s * 8, 8)
            pltpu.make_async_copy(
                tables.at[:, pl.ds(row, 8), :], blocks.at[e % 2, :, pl.ds(slot, 8), :], sem.at[e % 2]).start()
            return 0

        lax.fori_loop(0, cnt_ref[e] * PICK, body, 0)

    issue(0)
    for e in range(n_emb):
        buf = e % 2
        if e + 1 < n_emb:
            issue(e + 1)

        def drain(s, _):
            pltpu.make_async_copy(
                tables.at[:, pl.ds(0, 8 * PICK), :], blocks.at[buf, :, pl.ds(0, 8 * PICK), :], sem.at[buf]).wait()
            return 0

        lax.fori_loop(0, cnt_ref[e], drain, 0)

        def take(b, _):
            r = pl.multiple_of(b * PICK, PICK)
            pick = pick_ref[pl.ds(pl.multiple_of(e * cap + r, PICK), PICK), :]
            for l in range(n_layers):
                rows = blocks[buf, l, pl.ds(pl.multiple_of(r * 8, 8 * PICK), 8 * PICK), :]
                rest[l * n_emb + e][pl.ds(r, PICK), :] = jnp.dot(pick, rows, preferred_element_type=F32).astype(BF)
            return 0

        lax.fori_loop(0, cnt_ref[e], take, 0)

        def blank(b, _):
            r = pl.multiple_of(b * PICK, PICK)
            for l in range(n_layers):
                rest[l * n_emb + e][pl.ds(r, PICK), :] = jnp.zeros((PICK, tables.shape[2]), BF)
            return 0

        lax.fori_loop(cnt_ref[e], cap // PICK, blank, 0)


def serve_rows(tables, counts, starts, ids, pick, cap):
    n_layers, _, width = tables.shape
    n_emb = counts.shape[0]
    smem = pl.BlockSpec(memory_space=pltpu.SMEM)
    vmem = pl.BlockSpec(memory_space=pltpu.VMEM)
    return pl.pallas_call(
        functools.partial(serve_kernel, n_layers, cap),
        out_shape=[jax.ShapeDtypeStruct((cap, width), BF)] * (n_layers * n_emb),
        in_specs=[smem, smem, smem, vmem, pl.BlockSpec(memory_space=pltpu.HBM)],
        out_specs=[vmem] * (n_layers * n_emb),
        scratch_shapes=[
            pltpu.VMEM((2, n_layers, cap * 8, width), BF),
            pltpu.SemaphoreType.DMA((2,)),
        ],
        compiler_params=pltpu.CompilerParams(vmem_limit_bytes=48 << 20),
        cost_estimate=pl.CostEstimate(flops=20_000_000_000, bytes_accessed=30_000_000, transcendentals=0),
        name="serve_rows",
    )(counts, starts, ids, pick, *in_hbm(tables))


N_SRC = 16
MAX_ROWS = 17 * BLK


def pull_runs(meta_ref, srcs, col, dst, sem):
    width = dst.shape[1]

    def run(src, k, base):
        lo, off = meta_ref[k], meta_ref[2 * N_SRC + k]

        def chunk(c, _):
            a = pl.multiple_of(base + lo + c * CHUNK, CHUNK)
            b = pl.multiple_of((off + c) * CHUNK, CHUNK)
            pltpu.make_async_copy(src.at[pl.ds(a, CHUNK), col:col + width], dst.at[pl.ds(b, CHUNK), :], sem).start()
            return 0

        lax.fori_loop(0, meta_ref[N_SRC + k], chunk, 0)

    if len(srcs) == 1:
        src_rows = srcs[0].shape[0] // N_SRC
        lax.fori_loop(0, N_SRC, lambda k, c: (run(srcs[0], k, k * src_rows), c)[1], 0)
    else:
        for j, src in enumerate(srcs):
            run(src, meta_ref[3 * N_SRC + 1 + j], 0)


def drain_runs(meta_ref, srcs, col, dst, sem):
    width = dst.shape[1]

    def one(c, _):
        pltpu.make_async_copy(srcs[0].at[pl.ds(0, CHUNK), col:col + width], dst.at[pl.ds(0, CHUNK), :], sem).wait()
        return 0

    lax.fori_loop(0, meta_ref[3 * N_SRC], one, 0)


def n_blocks(meta_ref):
    return lax.div(meta_ref[3 * N_SRC] * CHUNK + BLK - 1, BLK)


def gate_kernel(layer, col, meta_ref, u_hbm, w_ref, out, uc, stage, sem_u, sem_o):
    pull_runs(meta_ref, [u_hbm], col, uc, sem_u)
    drain_runs(meta_ref, [u_hbm], col, uc, sem_u)
    total = n_blocks(meta_ref)

    def out_copy(b):
        buf = lax.rem(b, 2)
        return pltpu.make_async_copy(stage.at[buf], out.at[pl.ds(b * (BLK // 8), BLK // 8)], sem_o.at[buf])

    def block(b, _):
        @pl.when(b >= 2)
        def _():
            out_copy(b - 2).wait()

        u = uc[pl.ds(pl.multiple_of(b * BLK, BLK), BLK), :]
        for n in range(4):
            pre = jnp.dot(u, w_ref[layer, :, n * 256:(n + 1) * 256], preferred_element_type=F32)
            act = jax.nn.gelu(pre)
            for j in range(2):
                stage[lax.rem(b, 2), :, n * 2 + j] = act[:, j * 128:(j + 1) * 128].reshape(BLK // 8, 8, 128)
        out_copy(b).start()
        return 0

    lax.fori_loop(0, total, block, 0)
    lax.fori_loop(jnp.maximum(total - 2, 0), total, lambda b, c: (out_copy(b).wait(), c)[1], 0)


def owner_gate(layer, meta, u_all, col, w_gate):
    smem = pl.BlockSpec(memory_space=pltpu.SMEM)
    hbm = pl.BlockSpec(memory_space=pltpu.HBM)
    width = w_gate.shape[2]
    return pl.pallas_call(
        functools.partial(gate_kernel, layer, col),
        out_shape=pltpu.HBM((MAX_ROWS // 8, width // 128, 8, 128), F32),
        in_specs=[smem, hbm, pl.BlockSpec(memory_space=pltpu.VMEM)],
        out_specs=hbm,
        scratch_shapes=[
            pltpu.VMEM((MAX_ROWS, width), BF),
            pltpu.VMEM((2, BLK // 8, width // 128, 8, 128), F32),
            pltpu.SemaphoreType.DMA,
            pltpu.SemaphoreType.DMA((2,)),
        ],
        compiler_params=pltpu.CompilerParams(vmem_limit_bytes=28 << 20),
        cost_estimate=pl.CostEstimate(flops=10_000_000_000, bytes_accessed=30_000_000, transcendentals=0),
    )(meta, *in_hbm(u_all), w_gate)


UNROLL = 8


def owner_kernel(layer, col, n_src, meta_ref, tile_ref, addr_ref, g_hbm, *rest):
    d_hbm = rest[:n_src]
    out, dc, prod, acc, sem_d, sem_g, sem_o = rest[-7:]
    n_tiles = tile_ref.shape[0] - 1
    total = n_blocks(meta_ref)

    def g_copy(b):
        n = BLK // 8
        return pltpu.make_async_copy(
            g_hbm.at[pl.ds(b * n, n)], prod.reshape(MAX_ROWS // 8, 8, 8, 128).at[pl.ds(b * n, n)], sem_g.at[b])

    pull_runs(meta_ref, d_hbm, col, dc, sem_d)
    lax.fori_loop(0, total, lambda b, c: (g_copy(b).start(), c)[1], 0)

    def clear(buf):
        def some(i, _):
            acc[buf, pl.ds(pl.multiple_of(i * 512, 512), 512), :] = jnp.zeros((512, 128), F32)
            return 0

        lax.fori_loop(0, TILE_ROWS * 8 // 512, some, 0)

    clear(0)
    clear(1)
    drain_runs(meta_ref, d_hbm, col, dc, sem_d)

    def block(b, _):
        g_copy(b).wait()
        for t in range(BLK // 16):
            d = dc[pl.ds(pl.multiple_of(b * BLK + t * 16, 16), 16), :].astype(F32)
            for h in range(2):
                for j in range(8):
                    at = pl.ds(pl.multiple_of(b * (BLK * 8) + (2 * t + h) * 64 + j * 8, 8), 8)
                    prod[at, :] = prod[at, :] * d[h * 8:(h + 1) * 8, j * 128:(j + 1) * 128]
        return 0

    lax.fori_loop(0, total, block, 0)

    def out_copy(t, buf):
        return pltpu.make_async_copy(
            acc.at[buf].reshape(TILE_ROWS // 8, 8, 8, 128),
            out.at[layer, pl.ds(t * (TILE_ROWS // 8), TILE_ROWS // 8)], sem_o.at[buf])

    def tile(t, _):
        buf = lax.rem(t, 2)

        @pl.when(t >= 2)
        def _():
            out_copy(t - 2, buf).wait()
            clear(buf)

        first, last = tile_ref[t], tile_ref[t + 1]

        def one(i, run):
            word = addr_ref[i]
            pa = lax.bitwise_and(word, 0xFFFF)
            ra = lax.bitwise_and(lax.shift_right_logical(word, 16), 0x1FFF)
            fresh = word >= (1 << 29)
            run = jnp.where(fresh, 0.0, run) + prod[pl.ds(pa, 8, stride=8), :]
            acc[buf, pl.ds(ra, 8, stride=8), :] = run
            return run

        def many(i, run):
            for u in range(UNROLL):
                run = one(first + i * UNROLL + u, run)
            return run

        groups = lax.div(last - first, UNROLL)
        run = lax.fori_loop(0, groups, many, jnp.zeros((8, 128), F32))
        lax.fori_loop(first + groups * UNROLL, last, one, run)
        out_copy(t, buf).start()
        return 0

    lax.fori_loop(0, n_tiles, tile, 0)
    out_copy(n_tiles - 2, n_tiles % 2).wait()
    out_copy(n_tiles - 1, (n_tiles - 1) % 2).wait()


def owner_grad(layer, out_prev, out_shape, meta, tiles, addrs, g_rows, d_all, col):
    smem = pl.BlockSpec(memory_space=pltpu.SMEM)
    hbm = pl.BlockSpec(memory_space=pltpu.HBM)
    width = g_rows.shape[1] * 128
    args = [meta, tiles, addrs, *in_hbm(g_rows, *d_all)]
    specs = [smem, smem, smem, hbm] + [hbm] * len(d_all)
    aliases = {}
    if out_prev is not None:
        args.append(out_prev)
        specs.append(hbm)
        aliases = {len(args) - 1: 0}
    return pl.pallas_call(
        functools.partial(owner_kernel, layer, col, len(d_all)),
        out_shape=jax.ShapeDtypeStruct(out_shape, F32),
        in_specs=specs,
        out_specs=hbm,
        scratch_shapes=[
            pltpu.VMEM((MAX_ROWS, width), BF),
            pltpu.VMEM((MAX_ROWS * 8, 128), F32),
            pltpu.VMEM((2, TILE_ROWS * 8, 128), F32),
            pltpu.SemaphoreType.DMA,
            pltpu.SemaphoreType.DMA((MAX_ROWS // BLK,)),
            pltpu.SemaphoreType.DMA((2,)),
        ],
        input_output_aliases=aliases,
        compiler_params=pltpu.CompilerParams(vmem_limit_bytes=48 << 20),
        cost_estimate=pl.CostEstimate(flops=40_000_000_000, bytes_accessed=100_000_000, transcendentals=0),
    )(*args)


def solution(mesh):
    n_emb = mesh.shape['emb']
    n_dev = n_emb * mesh.shape['dp']
    tok_spec = P(('dp', 'emb'))
    act_spec = P(('dp', 'emb'), None)
    table_spec = P(None, 'emb', None)
    full_spec = P(None, None, None)
    everyone = ('dp', 'emb')

    def device_body(tok_ids, resid_in, cot_out, tables, w_up, w_down, w_gate, w_proj):
        n_layers, range_rows, width = tables.shape
        n_dp = n_dev // n_emb
        n_tok = tok_ids.shape[0]
        cap = min(2 * n_tok // n_emb, 3 * n_tok // 4)
        i_dp, i_emb = lax.axis_index('dp'), lax.axis_index('emb')
        last = n_layers - 1

        def gather(rows):
            return lax.all_gather(rows, everyone, axis=0, tiled=True)

        pos = jnp.arange(n_tok, dtype=jnp.int32)
        before = (tok_ids[None, :] < tok_ids[:, None]) | ((tok_ids[None, :] == tok_ids[:, None]) & (pos[None, :] < pos[:, None]))
        rank = jnp.sum(before.astype(jnp.int32), axis=1)
        perm_mask = rank[None, :] == pos[:, None]
        perm = perm_mask.astype(BF)
        x = jnp.dot(perm, resid_in, preferred_element_type=F32).astype(BF)
        cot = jnp.dot(perm, cot_out, preferred_element_type=F32).astype(BF)
        normed = rms_norm(x.astype(F32)).astype(BF)
        d_mixed = lax.dot_general(cot, w_proj[last], (((1,), (1,)), ((), ())), preferred_element_type=F32).astype(BF)
        set_a = gather(normed)

        def flip(block, axis, bit):
            n = mesh.shape[axis]
            return lax.ppermute(block, axis, [(i, i ^ bit) for i in range(n)])

        def spread(block):
            at = {(0, 0, 0): block}
            at[1, 0, 0] = flip(block, 'emb', 2)
            at[0, 1, 0] = flip(block, 'dp', 1)
            at[0, 0, 1] = flip(block, 'dp', 2)
            at[0, 1, 1] = flip(at[0, 1, 0], 'dp', 2)
            at[1, 0, 1] = flip(at[1, 0, 0], 'dp', 2)
            at[1, 1, 0] = flip(at[1, 0, 0], 'dp', 1)
            at[1, 1, 1] = flip(at[1, 0, 1], 'dp', 1)
            offsets = sorted(at, key=lambda o: (sum(o), o))
            blocks = [at[o] for o in offsets] + [flip(at[o], 'emb', 1) for o in offsets]
            places = [((o[2] * 2 + o[1]), (o[0] * 2 + c)) for c in range(2) for o in offsets]
            return blocks, places

        d2_blocks, places = spread(d_mixed)
        sources = jnp.stack([(i_dp ^ d) * n_emb + (i_emb ^ e) for d, e in places]).astype(jnp.int32)

        ids = jnp.sum(jnp.where(perm_mask, tok_ids[None, :], 0), axis=1)
        ids, _ = lax.optimization_barrier((ids, d_mixed))
        ids_all = share_ids(ids, n_dp, n_emb)
        ids_2d = ids_all.reshape(n_dev, n_tok)
        base = i_emb * range_rows

        peers = i_dp * n_emb + (i_emb ^ jnp.arange(n_emb, dtype=jnp.int32))
        is_peer = peers[:, None] == jnp.arange(n_dev, dtype=jnp.int32)[None, :]
        mine = jnp.sum(jnp.where(is_peer[:, :, None], ids_2d[None], 0), axis=1)
        peer_lo = jnp.sum((mine < base).astype(jnp.int32), axis=1)
        count = jnp.sum((mine < base + range_rows).astype(jnp.int32), axis=1) - peer_lo
        slot_pos = jnp.arange(cap, dtype=jnp.int32)
        at = pos[None, None, :] == (peer_lo[:, None] + slot_pos[None, :])[:, :, None]
        low = jnp.sum(jnp.where(at, mine[:, None, :] % 8, 0), axis=2)
        pick_col = jnp.where(slot_pos[None, :] < count[:, None], (slot_pos[None, :] % PICK) * 8 + low, -1)
        pick8 = (pick_col.reshape(-1, 1) == jnp.arange(8 * PICK, dtype=jnp.int32)[None, :]).astype(BF)
        served = serve_rows(tables, (count + PICK - 1) // PICK, peer_lo + peers * n_tok,
                            jnp.pad(ids_all, (0, PICK)), pick8, cap)
        returned = [[served[l * n_emb]] + [flip(served[l * n_emb + f], 'emb', f) for f in range(1, n_emb)]
                    for l in range(n_layers)]
        owner = ids // range_rows
        first = jnp.sum((owner[None, :] < owner[:, None]).astype(jnp.int32), axis=1)
        slot = (owner ^ i_emb) * cap + pos - first
        pick = (slot[:, None] == jnp.arange(n_emb * cap, dtype=jnp.int32)[None, :]).astype(BF)

        weights = (w_up, w_down, w_gate, w_proj)
        saved, us = [], [normed]
        for l in range(n_layers):
            x_in = x
            x, u_next, *kept = layer_fwd(l, l > 0, x, us[-1], returned[l], pick, *weights)
            saved.append((x_in, *kept))
            us.append(u_next)
        set_b = gather(jnp.concatenate(us[1:n_layers], axis=1))
        resid_out = lax.dot_general(perm, x, (((0,), (0,)), ((), ())), preferred_element_type=F32).astype(BF)
        d_sets = [None] * n_layers
        for l in range(last, 0, -1):
            x_in, up_pre, gate_pre, got = saved[l]
            cot, d_mixed = layer_bwd(l, cot, d_mixed, x_in, got, up_pre, gate_pre, *weights)
            d_sets[l - 1] = spread(d_mixed)[0] if l == last else [gather(d_mixed)]

        n_tiles = range_rows // TILE_ROWS
        lo = jnp.sum((ids_2d < base).astype(jnp.int32), axis=1)
        hi = jnp.sum((ids_2d < base + range_rows).astype(jnp.int32), axis=1)
        lo16 = (lo // CHUNK) * CHUNK
        n_ch = (hi - lo16 + CHUNK - 1) // CHUNK
        tri = jnp.arange(n_dev)[None, :] < jnp.arange(n_dev)[:, None]
        off = jnp.sum(jnp.where(tri, n_ch[None, :], 0), axis=1)
        meta = jnp.concatenate([lo16, n_ch, off, jnp.sum(n_ch)[None], sources]).astype(jnp.int32)
        place = (off * CHUNK - lo16)[:, None] + pos[None, :]
        local = ids_2d - base
        owned = (local >= 0) & (local < range_rows)
        key = jnp.where(owned, local * (1 << 13) + place, jnp.iinfo(jnp.int32).max)
        key = lax.sort(key.reshape(-1), is_stable=False)[:n_emb * n_dev * cap // 4]
        p, r = key & ((1 << 13) - 1), key >> 13
        fresh = jnp.concatenate([jnp.ones((1,), jnp.bool_), r[1:] != r[:-1]])
        in_tile = r % TILE_ROWS
        addrs = ((p // 8) * 64 + p % 8) | (((in_tile // 8) * 64 + in_tile % 8) << 16) | (fresh.astype(jnp.int32) << 29)
        edges = jnp.arange(n_tiles + 1, dtype=jnp.int32) * TILE_ROWS
        tiles = jnp.sum((r[None, :] < edges[:, None]).astype(jnp.int32), axis=1)

        set_a, _ = lax.optimization_barrier((set_a, d_mixed))
        u_sets = [(set_a, 0)] + [(set_b, i * width) for i in range(n_layers - 1)]
        d_sets[last] = d2_blocks
        grads = None
        out_shape = (n_layers, range_rows // 8, width // 128, 8, 128)
        gates = []
        for l in range(n_layers):
            gates.append(owner_gate(l, meta, *u_sets[l], w_gate))
        for l in range(last, -1, -1):
            grads = owner_grad(l, grads, out_shape, meta, tiles, addrs, gates[l], d_sets[l], 0)
        d_tables = grads.transpose(0, 1, 3, 2, 4).reshape(n_layers, range_rows, width)
        return resid_out, d_tables

    return jax.shard_map(device_body, mesh=mesh, in_specs=(tok_spec, act_spec, act_spec, table_spec, full_spec, full_spec, full_spec, full_spec), out_specs=(act_spec, table_spec), check_vma=False)
```

```python
import functools

import jax
import jax.numpy as jnp
from jax import lax
from jax.experimental import pallas as pl
from jax.experimental.pallas import tpu as pltpu
from jax.sharding import PartitionSpec as P


NORM_EPS = 1e-6
BF = jnp.bfloat16
F32 = jnp.float32

CHUNK = 16
BLK = 256
TILE_ROWS = 1024


def in_hbm(*arrays):
    return [pltpu.with_memory_space_constraint(a, pltpu.HBM) for a in arrays]


def rms_norm(x_f32):
    return x_f32 * lax.rsqrt(jnp.mean(x_f32 * x_f32, axis=-1, keepdims=True) + NORM_EPS)


def share_kernel(n_dp, n_emb, ids_ref, out_ref, local_sem, send_sem, recv_sem):
    n = n_dp * n_emb
    me = lax.axis_index('dp') * n_emb + lax.axis_index('emb')

    def place(o):
        to = lax.rem(me + o, n)
        return (to // n_emb, lax.rem(to, n_emb))

    barrier = pltpu.get_barrier_semaphore()
    for o in range(1, n):
        pl.semaphore_signal(barrier, inc=1, device_id=place(o), device_id_type=pl.DeviceIdType.MESH)
    pl.semaphore_wait(barrier, n - 1)
    sends = [
        pltpu.make_async_remote_copy(
            src_ref=ids_ref, dst_ref=out_ref.at[me], send_sem=send_sem.at[o], recv_sem=recv_sem.at[o],
            device_id=place(o), device_id_type=pl.DeviceIdType.MESH)
        for o in range(1, n)
    ]
    for cp in sends:
        cp.start()
    out_ref[me] = ids_ref[...]
    for cp in sends:
        cp.wait()


def share_ids(ids, n_dp, n_emb):
    n = n_dp * n_emb
    rows = ids.shape[0] // 128
    vmem = pl.BlockSpec(memory_space=pltpu.VMEM)
    out = pl.pallas_call(
        functools.partial(share_kernel, n_dp, n_emb),
        out_shape=jax.ShapeDtypeStruct((n, rows, 128), jnp.int32),
        in_specs=[vmem], out_specs=vmem,
        scratch_shapes=[pltpu.SemaphoreType.DMA, pltpu.SemaphoreType.DMA((n,)), pltpu.SemaphoreType.DMA((n,))],
        compiler_params=pltpu.CompilerParams(collective_id=0, has_side_effects=True),
        name="share_ids",
    )(ids.reshape(rows, 128))
    return out.reshape(-1)


FCH = 512
N_BUF = 3
GELU_C = 0.7978845608028654
GELU_A = 0.044715


def gelu_grad(v):
    t = jnp.tanh(GELU_C * (v + GELU_A * (v * v * v)))
    return 0.5 * (1.0 + t) + (0.5 * GELU_C) * v * (1.0 - t * t) * (1.0 + (3 * GELU_A) * (v * v))


def dot_nt(a, b):
    return lax.dot_general(a, b, (((1,), (1,)), ((), ())), preferred_element_type=F32)


def dot_nn(a, b):
    return jnp.dot(a, b, preferred_element_type=F32)


def stream(layer, w_up, w_down, up_buf, down_buf, sem):
    def copies(c):
        buf = lax.rem(c, N_BUF)
        f = pl.multiple_of(c * FCH, FCH)
        return (pltpu.make_async_copy(w_up.at[layer, :, pl.ds(f, FCH)], up_buf.at[buf], sem.at[0, buf]),
                pltpu.make_async_copy(w_down.at[layer, pl.ds(f, FCH), :], down_buf.at[buf], sem.at[1, buf]))

    return copies


def forward_kernel(layer, keep, x_ref, u_ref, r0_ref, r1_ref, r2_ref, r3_ref, pick_ref, w_up, w_down, w_gate, w_proj, *rest):
    if keep:
        x_out, u_out, up_hbm, gate_hbm, got_out = rest[:5]
        up_buf, down_buf, gate_w, proj_w, acc, up_stage, gate_stage, sem, sem_gp, sem_o = rest[5:]
    else:
        x_out, u_out = rest[:2]
        up_buf, down_buf, gate_w, proj_w, acc, sem, sem_gp = rest[2:]
    n_ch = w_up.shape[2] // FCH
    copies = stream(layer, w_up, w_down, up_buf, down_buf, sem)
    for c in range(N_BUF - 1):
        for cp in copies(c):
            cp.start()
    gate_cp = pltpu.make_async_copy(w_gate.at[layer], gate_w, sem_gp.at[0])
    proj_cp = pltpu.make_async_copy(w_proj.at[layer], proj_w, sem_gp.at[1])
    gate_cp.start()
    proj_cp.start()

    def stage_copy(c):
        buf = lax.rem(c, 2)
        return pltpu.make_async_copy(
            up_stage.at[buf], up_hbm.at[:, pl.ds(pl.multiple_of(c * FCH, FCH), FCH)], sem_o.at[buf])

    acc[...] = x_ref[...].astype(F32)

    def chunk(c, _):
        @pl.when(c + N_BUF - 1 < n_ch)
        def _():
            for cp in copies(c + N_BUF - 1):
                cp.start()

        for cp in copies(c):
            cp.wait()
        if keep:
            @pl.when(c >= 2)
            def _():
                stage_copy(c - 2).wait()

        buf = lax.rem(c, N_BUF)
        hidden = []
        for n in range(FCH // 256):
            pre = dot_nn(u_ref[...], up_buf[buf, :, n * 256:(n + 1) * 256])
            if keep:
                up_stage[lax.rem(c, 2), :, n * 256:(n + 1) * 256] = pre
            hidden.append(jax.nn.gelu(pre).astype(BF))
        hidden = jnp.concatenate(hidden, axis=1)
        for n in range(4):
            acc[:, n * 256:(n + 1) * 256] += dot_nn(hidden, down_buf[buf, :, n * 256:(n + 1) * 256])
        if keep:
            stage_copy(c).start()
        return 0

    lax.fori_loop(0, n_ch, chunk, 0)
    gate_cp.wait()
    proj_cp.wait()
    mixed = []
    for n in range(4):
        cols = slice(n * 256, (n + 1) * 256)
        pre = dot_nn(u_ref[...], gate_w[:, cols])
        cap = r0_ref.shape[0]
        got = sum(dot_nn(pick_ref[:, f * cap:(f + 1) * cap], r[:, cols])
                  for f, r in enumerate((r0_ref, r1_ref, r2_ref, r3_ref))).astype(BF)
        if keep:
            gate_stage[:, cols] = pre
            got_out[:, cols] = got
        mixed.append((jax.nn.gelu(pre) * got.astype(F32)).astype(BF))
    mixed = jnp.concatenate(mixed, axis=1)
    if keep:
        gate_out = pltpu.make_async_copy(gate_stage, gate_hbm, sem_o.at[2])
        gate_out.start()
    for n in range(4):
        cols = slice(n * 256, (n + 1) * 256)
        x_out[:, cols] = (acc[:, cols] + dot_nn(mixed, proj_w[:, cols])).astype(BF)
    x_next = x_out[...].astype(F32)
    scale = lax.rsqrt(jnp.mean(x_next * x_next, axis=-1, keepdims=True) + NORM_EPS)
    u_out[...] = (x_next * scale).astype(BF)
    if keep:
        gate_out.wait()
        stage_copy(n_ch - 2).wait()
        stage_copy(n_ch - 1).wait()


def layer_fwd(layer, keep, x, u, rows, pick, w_up, w_down, w_gate, w_proj):
    t, d = x.shape
    f = w_up.shape[2]
    hbm = pl.BlockSpec(memory_space=pltpu.HBM)
    vmem = pl.BlockSpec(memory_space=pltpu.VMEM)
    act = jax.ShapeDtypeStruct((t, d), BF)
    out_shape = [act, act]
    out_specs = [vmem, vmem]
    scratch = [
        pltpu.VMEM((N_BUF, d, FCH), BF), pltpu.VMEM((N_BUF, FCH, d), BF),
        pltpu.VMEM((d, d), BF), pltpu.VMEM((d, d), BF), pltpu.VMEM((t, d), F32),
    ]
    sems = [pltpu.SemaphoreType.DMA((2, N_BUF)), pltpu.SemaphoreType.DMA((2,))]
    if keep:
        out_shape += [pltpu.HBM((t, f), F32), pltpu.HBM((t, d), F32), act]
        out_specs += [hbm, hbm, vmem]
        scratch += [pltpu.VMEM((2, t, FCH), F32), pltpu.VMEM((t, d), F32)]
        sems += [pltpu.SemaphoreType.DMA((3,))]
    return pl.pallas_call(
        functools.partial(forward_kernel, layer, keep),
        out_shape=out_shape, in_specs=[vmem] * 7 + [hbm] * 4, out_specs=out_specs,
        scratch_shapes=scratch + sems,
        compiler_params=pltpu.CompilerParams(vmem_limit_bytes=40 << 20),
        cost_estimate=pl.CostEstimate(flops=11_000_000_000, bytes_accessed=30_000_000, transcendentals=0),
    )(x, u, *rows, pick, *in_hbm(w_up, w_down, w_gate, w_proj))


def backward_kernel(layer, cot_ref, dm_ref, x_ref, got_ref, up_hbm, gate_hbm, w_up, w_down, w_gate, w_proj,
                    cot_out, dm_out, up_buf, down_buf, pre_buf, gate_w, proj_w, gate_pre, acc, sem, sem_gp):
    n_ch = w_up.shape[2] // FCH
    copies = stream(layer, w_up, w_down, up_buf, down_buf, sem)

    def all_copies(c):
        buf = lax.rem(c, N_BUF)
        pre = pltpu.make_async_copy(
            up_hbm.at[:, pl.ds(pl.multiple_of(c * FCH, FCH), FCH)], pre_buf.at[buf], sem.at[2, buf])
        return copies(c) + (pre,)

    for c in range(N_BUF - 1):
        for cp in all_copies(c):
            cp.start()
    gate_cp = pltpu.make_async_copy(w_gate.at[layer], gate_w, sem_gp.at[0])
    pre_cp = pltpu.make_async_copy(gate_hbm, gate_pre, sem_gp.at[1])
    proj_cp = pltpu.make_async_copy(w_proj.at[layer - 1], proj_w, sem_gp.at[2])
    for cp in (gate_cp, pre_cp, proj_cp):
        cp.start()

    def chunk(c, _):
        @pl.when(c + N_BUF - 1 < n_ch)
        def _():
            for cp in all_copies(c + N_BUF - 1):
                cp.start()

        for cp in all_copies(c):
            cp.wait()
        buf = lax.rem(c, N_BUF)
        d_pre = []
        for n in range(FCH // 256):
            cols = slice(n * 256, (n + 1) * 256)
            d_hidden = dot_nt(cot_ref[...], down_buf[buf, cols, :]).astype(BF).astype(F32)
            d_pre.append((d_hidden * gelu_grad(pre_buf[buf, :, cols])).astype(BF))
        d_pre = jnp.concatenate(d_pre, axis=1)
        for n in range(4):
            cols = slice(n * 256, (n + 1) * 256)
            part = dot_nt(d_pre, up_buf[buf, cols, :])
            acc[:, cols] = part + jnp.where(c == 0, 0.0, acc[:, cols])
        return 0

    lax.fori_loop(0, n_ch, chunk, 0)
    for cp in (gate_cp, pre_cp, proj_cp):
        cp.wait()
    d_pre = []
    for n in range(4):
        cols = slice(n * 256, (n + 1) * 256)
        d_act = dm_ref[:, cols].astype(F32) * got_ref[:, cols].astype(F32)
        d_pre.append((d_act * gelu_grad(gate_pre[:, cols])).astype(BF))
    d_pre = jnp.concatenate(d_pre, axis=1)
    for n in range(4):
        cols = slice(n * 256, (n + 1) * 256)
        both = acc[:, cols].astype(BF) + dot_nt(d_pre, gate_w[cols, :]).astype(BF)
        acc[:, cols] = both.astype(F32)
    x = x_ref[...].astype(F32)
    dy = acc[...]
    r = lax.rsqrt(jnp.mean(x * x, axis=-1, keepdims=True) + NORM_EPS)
    proj = jnp.mean(x * dy, axis=-1, keepdims=True)
    cot = (cot_ref[...].astype(F32) + (dy * r - x * (r * r * r * proj))).astype(BF)
    cot_out[...] = cot
    for n in range(4):
        cols = slice(n * 256, (n + 1) * 256)
        dm_out[:, cols] = dot_nt(cot, proj_w[cols, :]).astype(BF)


def layer_bwd(layer, cot, d_mixed, x, got, up_pre, gate_pre, w_up, w_down, w_gate, w_proj):
    t, d = x.shape
    hbm = pl.BlockSpec(memory_space=pltpu.HBM)
    vmem = pl.BlockSpec(memory_space=pltpu.VMEM)
    act = jax.ShapeDtypeStruct((t, d), BF)
    return pl.pallas_call(
        functools.partial(backward_kernel, layer),
        out_shape=[act, act], in_specs=[vmem] * 4 + [hbm] * 6, out_specs=[vmem, vmem],
        scratch_shapes=[
            pltpu.VMEM((N_BUF, d, FCH), BF), pltpu.VMEM((N_BUF, FCH, d), BF), pltpu.VMEM((N_BUF, t, FCH), F32),
            pltpu.VMEM((d, d), BF), pltpu.VMEM((d, d), BF), pltpu.VMEM((t, d), F32), pltpu.VMEM((t, d), F32),
            pltpu.SemaphoreType.DMA((3, N_BUF)), pltpu.SemaphoreType.DMA((3,)),
        ],
        compiler_params=pltpu.CompilerParams(vmem_limit_bytes=40 << 20),
        cost_estimate=pl.CostEstimate(flops=11_000_000_000, bytes_accessed=40_000_000, transcendentals=0),
    )(cot, d_mixed, x, got, *in_hbm(up_pre, gate_pre, w_up, w_down, w_gate, w_proj))


PICK = 32


def serve_kernel(n_layers, cap, cnt_ref, start_ref, ids_ref, pick_ref, tables, *rest):
    blocks, sem = rest[-2:]
    n_emb = len(rest[:-2]) // n_layers
    range_rows = tables.shape[1]

    def issue(e):
        def body(s, _):
            row = lax.rem(ids_ref[start_ref[e] + s], range_rows)
            row = pl.multiple_of(lax.div(row, 8) * 8, 8)
            slot = pl.multiple_of(s * 8, 8)
            pltpu.make_async_copy(
                tables.at[:, pl.ds(row, 8), :], blocks.at[e % 2, :, pl.ds(slot, 8), :], sem.at[e % 2]).start()
            return 0

        lax.fori_loop(0, cnt_ref[e] * PICK, body, 0)

    issue(0)
    for e in range(n_emb):
        buf = e % 2
        if e + 1 < n_emb:
            issue(e + 1)

        def drain(s, _):
            pltpu.make_async_copy(
                tables.at[:, pl.ds(0, 8 * PICK), :], blocks.at[buf, :, pl.ds(0, 8 * PICK), :], sem.at[buf]).wait()
            return 0

        lax.fori_loop(0, cnt_ref[e], drain, 0)

        def take(b, _):
            r = pl.multiple_of(b * PICK, PICK)
            pick = pick_ref[pl.ds(pl.multiple_of(e * cap + r, PICK), PICK), :]
            for l in range(n_layers):
                rows = blocks[buf, l, pl.ds(pl.multiple_of(r * 8, 8 * PICK), 8 * PICK), :]
                rest[l * n_emb + e][pl.ds(r, PICK), :] = jnp.dot(pick, rows, preferred_element_type=F32).astype(BF)
            return 0

        lax.fori_loop(0, cnt_ref[e], take, 0)

        def blank(b, _):
            r = pl.multiple_of(b * PICK, PICK)
            for l in range(n_layers):
                rest[l * n_emb + e][pl.ds(r, PICK), :] = jnp.zeros((PICK, tables.shape[2]), BF)
            return 0

        lax.fori_loop(cnt_ref[e], cap // PICK, blank, 0)


def serve_rows(tables, counts, starts, ids, pick, cap):
    n_layers, _, width = tables.shape
    n_emb = counts.shape[0]
    smem = pl.BlockSpec(memory_space=pltpu.SMEM)
    vmem = pl.BlockSpec(memory_space=pltpu.VMEM)
    return pl.pallas_call(
        functools.partial(serve_kernel, n_layers, cap),
        out_shape=[jax.ShapeDtypeStruct((cap, width), BF)] * (n_layers * n_emb),
        in_specs=[smem, smem, smem, vmem, pl.BlockSpec(memory_space=pltpu.HBM)],
        out_specs=[vmem] * (n_layers * n_emb),
        scratch_shapes=[
            pltpu.VMEM((2, n_layers, cap * 8, width), BF),
            pltpu.SemaphoreType.DMA((2,)),
        ],
        compiler_params=pltpu.CompilerParams(vmem_limit_bytes=48 << 20),
        cost_estimate=pl.CostEstimate(flops=20_000_000_000, bytes_accessed=30_000_000, transcendentals=0),
        name="serve_rows",
    )(counts, starts, ids, pick, *in_hbm(tables))


N_SRC = 16
MAX_ROWS = 17 * BLK


def pull_runs(meta_ref, srcs, col, dst, sem):
    width = dst.shape[1]

    def run(src, k, base):
        lo, off = meta_ref[k], meta_ref[2 * N_SRC + k]

        def chunk(c, _):
            a = pl.multiple_of(base + lo + c * CHUNK, CHUNK)
            b = pl.multiple_of((off + c) * CHUNK, CHUNK)
            pltpu.make_async_copy(src.at[pl.ds(a, CHUNK), col:col + width], dst.at[pl.ds(b, CHUNK), :], sem).start()
            return 0

        lax.fori_loop(0, meta_ref[N_SRC + k], chunk, 0)

    if len(srcs) == 1:
        src_rows = srcs[0].shape[0] // N_SRC
        lax.fori_loop(0, N_SRC, lambda k, c: (run(srcs[0], k, k * src_rows), c)[1], 0)
    else:
        for j, src in enumerate(srcs):
            run(src, meta_ref[3 * N_SRC + 1 + j], 0)


def drain_runs(meta_ref, srcs, col, dst, sem):
    width = dst.shape[1]

    def one(c, _):
        pltpu.make_async_copy(srcs[0].at[pl.ds(0, CHUNK), col:col + width], dst.at[pl.ds(0, CHUNK), :], sem).wait()
        return 0

    lax.fori_loop(0, meta_ref[3 * N_SRC], one, 0)


def n_blocks(meta_ref):
    return lax.div(meta_ref[3 * N_SRC] * CHUNK + BLK - 1, BLK)


def gate_kernel(layer, col, meta_ref, u_hbm, w_ref, out, uc, stage, sem_u, sem_o):
    pull_runs(meta_ref, [u_hbm], col, uc, sem_u)
    drain_runs(meta_ref, [u_hbm], col, uc, sem_u)
    total = n_blocks(meta_ref)

    def out_copy(b):
        buf = lax.rem(b, 2)
        return pltpu.make_async_copy(stage.at[buf], out.at[pl.ds(b * (BLK // 8), BLK // 8)], sem_o.at[buf])

    def block(b, _):
        @pl.when(b >= 2)
        def _():
            out_copy(b - 2).wait()

        u = uc[pl.ds(pl.multiple_of(b * BLK, BLK), BLK), :]
        for n in range(4):
            pre = jnp.dot(u, w_ref[layer, :, n * 256:(n + 1) * 256], preferred_element_type=F32)
            act = jax.nn.gelu(pre)
            for j in range(2):
                stage[lax.rem(b, 2), :, n * 2 + j] = act[:, j * 128:(j + 1) * 128].reshape(BLK // 8, 8, 128)
        out_copy(b).start()
        return 0

    lax.fori_loop(0, total, block, 0)
    lax.fori_loop(jnp.maximum(total - 2, 0), total, lambda b, c: (out_copy(b).wait(), c)[1], 0)


def owner_gate(layer, meta, u_all, col, w_gate):
    smem = pl.BlockSpec(memory_space=pltpu.SMEM)
    hbm = pl.BlockSpec(memory_space=pltpu.HBM)
    width = w_gate.shape[2]
    return pl.pallas_call(
        functools.partial(gate_kernel, layer, col),
        out_shape=pltpu.HBM((MAX_ROWS // 8, width // 128, 8, 128), F32),
        in_specs=[smem, hbm, pl.BlockSpec(memory_space=pltpu.VMEM)],
        out_specs=hbm,
        scratch_shapes=[
            pltpu.VMEM((MAX_ROWS, width), BF),
            pltpu.VMEM((2, BLK // 8, width // 128, 8, 128), F32),
            pltpu.SemaphoreType.DMA,
            pltpu.SemaphoreType.DMA((2,)),
        ],
        compiler_params=pltpu.CompilerParams(vmem_limit_bytes=28 << 20),
        cost_estimate=pl.CostEstimate(flops=10_000_000_000, bytes_accessed=30_000_000, transcendentals=0),
    )(meta, *in_hbm(u_all), w_gate)


UNROLL = 8


def owner_kernel(layer, col, n_src, meta_ref, tile_ref, addr_ref, g_hbm, *rest):
    d_hbm = rest[:n_src]
    out, dc, prod, acc, sem_d, sem_g, sem_o = rest[-7:]
    n_tiles = tile_ref.shape[0] - 1
    total = n_blocks(meta_ref)

    def g_copy(b):
        n = BLK // 8
        return pltpu.make_async_copy(
            g_hbm.at[pl.ds(b * n, n)], prod.reshape(MAX_ROWS // 8, 8, 8, 128).at[pl.ds(b * n, n)], sem_g.at[b])

    pull_runs(meta_ref, d_hbm, col, dc, sem_d)
    lax.fori_loop(0, total, lambda b, c: (g_copy(b).start(), c)[1], 0)

    def clear(buf):
        def some(i, _):
            acc[buf, pl.ds(pl.multiple_of(i * 512, 512), 512), :] = jnp.zeros((512, 128), F32)
            return 0

        lax.fori_loop(0, TILE_ROWS * 8 // 512, some, 0)

    clear(0)
    clear(1)
    drain_runs(meta_ref, d_hbm, col, dc, sem_d)

    def block(b, _):
        g_copy(b).wait()
        for t in range(BLK // 16):
            d = dc[pl.ds(pl.multiple_of(b * BLK + t * 16, 16), 16), :].astype(F32)
            for h in range(2):
                for j in range(8):
                    at = pl.ds(pl.multiple_of(b * (BLK * 8) + (2 * t + h) * 64 + j * 8, 8), 8)
                    prod[at, :] = prod[at, :] * d[h * 8:(h + 1) * 8, j * 128:(j + 1) * 128]
        return 0

    lax.fori_loop(0, total, block, 0)

    def out_copy(t, buf):
        return pltpu.make_async_copy(
            acc.at[buf].reshape(TILE_ROWS // 8, 8, 8, 128),
            out.at[layer, pl.ds(t * (TILE_ROWS // 8), TILE_ROWS // 8)], sem_o.at[buf])

    def tile(t, _):
        buf = lax.rem(t, 2)

        @pl.when(t >= 2)
        def _():
            out_copy(t - 2, buf).wait()
            clear(buf)

        first, last = tile_ref[t], tile_ref[t + 1]

        def one(i, run):
            word = addr_ref[i]
            pa = lax.bitwise_and(word, 0xFFFF)
            ra = lax.bitwise_and(lax.shift_right_logical(word, 16), 0x1FFF)
            fresh = word >= (1 << 29)
            run = jnp.where(fresh, 0.0, run) + prod[pl.ds(pa, 8, stride=8), :]
            acc[buf, pl.ds(ra, 8, stride=8), :] = run
            return run

        def many(i, run):
            for u in range(UNROLL):
                run = one(first + i * UNROLL + u, run)
            return run

        groups = lax.div(last - first, UNROLL)
        run = lax.fori_loop(0, groups, many, jnp.zeros((8, 128), F32))
        lax.fori_loop(first + groups * UNROLL, last, one, run)
        out_copy(t, buf).start()
        return 0

    lax.fori_loop(0, n_tiles, tile, 0)
    out_copy(n_tiles - 2, n_tiles % 2).wait()
    out_copy(n_tiles - 1, (n_tiles - 1) % 2).wait()


def owner_grad(layer, out_prev, out_shape, meta, tiles, addrs, g_rows, d_all, col):
    smem = pl.BlockSpec(memory_space=pltpu.SMEM)
    hbm = pl.BlockSpec(memory_space=pltpu.HBM)
    width = g_rows.shape[1] * 128
    args = [meta, tiles, addrs, *in_hbm(g_rows, *d_all)]
    specs = [smem, smem, smem, hbm] + [hbm] * len(d_all)
    aliases = {}
    if out_prev is not None:
        args.append(out_prev)
        specs.append(hbm)
        aliases = {len(args) - 1: 0}
    return pl.pallas_call(
        functools.partial(owner_kernel, layer, col, len(d_all)),
        out_shape=jax.ShapeDtypeStruct(out_shape, F32),
        in_specs=specs,
        out_specs=hbm,
        scratch_shapes=[
            pltpu.VMEM((MAX_ROWS, width), BF),
            pltpu.VMEM((MAX_ROWS * 8, 128), F32),
            pltpu.VMEM((2, TILE_ROWS * 8, 128), F32),
            pltpu.SemaphoreType.DMA,
            pltpu.SemaphoreType.DMA((MAX_ROWS // BLK,)),
            pltpu.SemaphoreType.DMA((2,)),
        ],
        input_output_aliases=aliases,
        compiler_params=pltpu.CompilerParams(vmem_limit_bytes=48 << 20),
        cost_estimate=pl.CostEstimate(flops=40_000_000_000, bytes_accessed=100_000_000, transcendentals=0),
    )(*args)


def solution(mesh):
    n_emb = mesh.shape['emb']
    n_dev = n_emb * mesh.shape['dp']
    tok_spec = P(('dp', 'emb'))
    act_spec = P(('dp', 'emb'), None)
    table_spec = P(None, 'emb', None)
    full_spec = P(None, None, None)
    everyone = ('dp', 'emb')

    def device_body(tok_ids, resid_in, cot_out, tables, w_up, w_down, w_gate, w_proj):
        n_layers, range_rows, width = tables.shape
        n_dp = n_dev // n_emb
        n_tok = tok_ids.shape[0]
        cap = min(2 * n_tok // n_emb, 3 * n_tok // 4)
        i_dp, i_emb = lax.axis_index('dp'), lax.axis_index('emb')
        last = n_layers - 1

        def gather(rows):
            return lax.all_gather(rows, everyone, axis=0, tiled=True)

        pos = jnp.arange(n_tok, dtype=jnp.int32)
        before = (tok_ids[None, :] < tok_ids[:, None]) | ((tok_ids[None, :] == tok_ids[:, None]) & (pos[None, :] < pos[:, None]))
        rank = jnp.sum(before.astype(jnp.int32), axis=1)
        perm_mask = rank[None, :] == pos[:, None]
        perm = perm_mask.astype(BF)
        x = jnp.dot(perm, resid_in, preferred_element_type=F32).astype(BF)
        normed = rms_norm(x.astype(F32)).astype(BF)
        u_sets = [gather(normed)]

        def flip(block, axis, bit):
            n = mesh.shape[axis]
            return lax.ppermute(block, axis, [(i, i ^ bit) for i in range(n)])

        def spread(block, x_heavy):
            at = {(0, 0, 0): block}
            at[1, 0, 0] = flip(block, 'emb', 2)
            at[0, 1, 0] = flip(block, 'dp', 1)
            at[0, 0, 1] = flip(block, 'dp', 2)
            at[0, 1, 1] = flip(at[0, 1, 0], 'dp', 2)
            if x_heavy:
                at[1, 0, 1] = flip(at[0, 0, 1], 'emb', 2)
                at[1, 1, 0] = flip(at[0, 1, 0], 'emb', 2)
            else:
                at[1, 0, 1] = flip(at[1, 0, 0], 'dp', 2)
                at[1, 1, 0] = flip(at[1, 0, 0], 'dp', 1)
            at[1, 1, 1] = flip(at[1, 0, 1], 'dp', 1)
            offsets = sorted(at, key=lambda o: (sum(o), o))
            blocks = [at[o] for o in offsets] + [flip(at[o], 'emb', 1) for o in offsets]
            places = [((o[2] * 2 + o[1]), (o[0] * 2 + c)) for c in range(2) for o in offsets]
            return blocks, places

        ids = jnp.sum(jnp.where(perm_mask, tok_ids[None, :], 0), axis=1)
        ids, _ = lax.optimization_barrier((ids, normed))
        ids_all = share_ids(ids, n_dp, n_emb)
        ids_2d = ids_all.reshape(n_dev, n_tok)
        base = i_emb * range_rows

        peers = i_dp * n_emb + (i_emb ^ jnp.arange(n_emb, dtype=jnp.int32))
        is_peer = peers[:, None] == jnp.arange(n_dev, dtype=jnp.int32)[None, :]
        mine = jnp.sum(jnp.where(is_peer[:, :, None], ids_2d[None], 0), axis=1)
        peer_lo = jnp.sum((mine < base).astype(jnp.int32), axis=1)
        count = jnp.sum((mine < base + range_rows).astype(jnp.int32), axis=1) - peer_lo
        slot_pos = jnp.arange(cap, dtype=jnp.int32)
        at = pos[None, None, :] == (peer_lo[:, None] + slot_pos[None, :])[:, :, None]
        low = jnp.sum(jnp.where(at, mine[:, None, :] % 8, 0), axis=2)
        pick_col = jnp.where(slot_pos[None, :] < count[:, None], (slot_pos[None, :] % PICK) * 8 + low, -1)
        pick8 = (pick_col.reshape(-1, 1) == jnp.arange(8 * PICK, dtype=jnp.int32)[None, :]).astype(BF)
        served = serve_rows(tables, (count + PICK - 1) // PICK, peer_lo + peers * n_tok,
                            jnp.pad(ids_all, (0, PICK)), pick8, cap)
        returned = [[served[l * n_emb]] + [flip(served[l * n_emb + f], 'emb', f) for f in range(1, n_emb)]
                    for l in range(n_layers)]
        owner = ids // range_rows
        first = jnp.sum((owner[None, :] < owner[:, None]).astype(jnp.int32), axis=1)
        slot = (owner ^ i_emb) * cap + pos - first
        pick = (slot[:, None] == jnp.arange(n_emb * cap, dtype=jnp.int32)[None, :]).astype(BF)

        cot_in, _ = lax.optimization_barrier((cot_out, served[0]))
        cot = jnp.dot(perm, cot_in, preferred_element_type=F32).astype(BF)
        d_mixed = lax.dot_general(cot, w_proj[last], (((1,), (1,)), ((), ())), preferred_element_type=F32).astype(BF)
        d_sets = [None] * n_layers
        d_sets[last], places = spread(d_mixed, False)
        sources = jnp.stack([(i_dp ^ d) * n_emb + (i_emb ^ e) for d, e in places]).astype(jnp.int32)

        n_tiles = range_rows // TILE_ROWS
        lo = jnp.sum((ids_2d < base).astype(jnp.int32), axis=1)
        hi = jnp.sum((ids_2d < base + range_rows).astype(jnp.int32), axis=1)
        lo16 = (lo // CHUNK) * CHUNK
        n_ch = (hi - lo16 + CHUNK - 1) // CHUNK
        tri = jnp.arange(n_dev)[None, :] < jnp.arange(n_dev)[:, None]
        off = jnp.sum(jnp.where(tri, n_ch[None, :], 0), axis=1)
        meta = jnp.concatenate([lo16, n_ch, off, jnp.sum(n_ch)[None], sources]).astype(jnp.int32)
        place = (off * CHUNK - lo16)[:, None] + pos[None, :]
        local = ids_2d - base
        owned = (local >= 0) & (local < range_rows)
        key = jnp.where(owned, local * (1 << 13) + place, jnp.iinfo(jnp.int32).max)
        key = lax.sort(key.reshape(-1), is_stable=False)[:n_emb * n_dev * cap // 4]
        p, r = key & ((1 << 13) - 1), key >> 13
        fresh = jnp.concatenate([jnp.ones((1,), jnp.bool_), r[1:] != r[:-1]])
        in_tile = r % TILE_ROWS
        addrs = ((p // 8) * 64 + p % 8) | (((in_tile // 8) * 64 + in_tile % 8) << 16) | (fresh.astype(jnp.int32) << 29)
        edges = jnp.arange(n_tiles + 1, dtype=jnp.int32) * TILE_ROWS
        tiles = jnp.sum((r[None, :] < edges[:, None]).astype(jnp.int32), axis=1)

        pick, meta, tiles, addrs = lax.optimization_barrier((pick, meta, tiles, addrs))

        weights = (w_up, w_down, w_gate, w_proj)
        saved, u = [], normed
        for l in range(n_layers):
            x_in = x
            x, u, *kept = layer_fwd(l, l > 0, x, u, returned[l], pick, *weights)
            saved.append((x_in, *kept))
            if l < last:
                u_sets.append(gather(u))
        resid_out = lax.dot_general(perm, x, (((0,), (0,)), ((), ())), preferred_element_type=F32).astype(BF)
        for l in range(last, 0, -1):
            x_in, up_pre, gate_pre, got = saved[l]
            cot, d_mixed = layer_bwd(l, cot, d_mixed, x_in, got, up_pre, gate_pre, *weights)
            d_sets[l - 1] = spread(d_mixed, True)[0] if l == last else [gather(d_mixed)]

        u_sets[0], _ = lax.optimization_barrier((u_sets[0], d_mixed))
        grads = None
        out_shape = (n_layers, range_rows // 8, width // 128, 8, 128)
        gates = []
        for l in range(n_layers):
            gates.append(owner_gate(l, meta, u_sets[l], 0, w_gate))
        for l in range(last, -1, -1):
            grads = owner_grad(l, grads, out_shape, meta, tiles, addrs, gates[l], d_sets[l], 0)
        d_tables = grads.transpose(0, 1, 3, 2, 4).reshape(n_layers, range_rows, width)
        return resid_out, d_tables

    return jax.shard_map(device_body, mesh=mesh, in_specs=(tok_spec, act_spec, act_spec, table_spec, full_spec, full_spec, full_spec, full_spec), out_specs=(act_spec, table_spec), check_vma=False)
```

```python
import functools

import jax
import jax.numpy as jnp
from jax import lax
from jax.experimental import pallas as pl
from jax.experimental.pallas import tpu as pltpu
from jax.sharding import PartitionSpec as P


NORM_EPS = 1e-6
BF = jnp.bfloat16
F32 = jnp.float32

CHUNK = 16
BLK = 256
TILE_ROWS = 1024


def in_hbm(*arrays):
    return [pltpu.with_memory_space_constraint(a, pltpu.HBM) for a in arrays]


def rms_norm(x_f32):
    return x_f32 * lax.rsqrt(jnp.mean(x_f32 * x_f32, axis=-1, keepdims=True) + NORM_EPS)


def share_kernel(n_dp, n_emb, ids_ref, out_ref, local_sem, send_sem, recv_sem):
    n = n_dp * n_emb
    me = lax.axis_index('dp') * n_emb + lax.axis_index('emb')

    def place(o):
        to = lax.rem(me + o, n)
        return (to // n_emb, lax.rem(to, n_emb))

    barrier = pltpu.get_barrier_semaphore()
    for o in range(1, n):
        pl.semaphore_signal(barrier, inc=1, device_id=place(o), device_id_type=pl.DeviceIdType.MESH)
    pl.semaphore_wait(barrier, n - 1)
    sends = [
        pltpu.make_async_remote_copy(
            src_ref=ids_ref, dst_ref=out_ref.at[me], send_sem=send_sem.at[o], recv_sem=recv_sem.at[o],
            device_id=place(o), device_id_type=pl.DeviceIdType.MESH)
        for o in range(1, n)
    ]
    for cp in sends:
        cp.start()
    out_ref[me] = ids_ref[...]
    for cp in sends:
        cp.wait()


def share_ids(ids, n_dp, n_emb):
    n = n_dp * n_emb
    rows = ids.shape[0] // 128
    vmem = pl.BlockSpec(memory_space=pltpu.VMEM)
    out = pl.pallas_call(
        functools.partial(share_kernel, n_dp, n_emb),
        out_shape=jax.ShapeDtypeStruct((n, rows, 128), jnp.int32),
        in_specs=[vmem], out_specs=vmem,
        scratch_shapes=[pltpu.SemaphoreType.DMA, pltpu.SemaphoreType.DMA((n,)), pltpu.SemaphoreType.DMA((n,))],
        compiler_params=pltpu.CompilerParams(collective_id=0, has_side_effects=True),
        name="share_ids",
    )(ids.reshape(rows, 128))
    return out.reshape(-1)


FCH = 512
N_BUF = 3
GELU_C = 0.7978845608028654
GELU_A = 0.044715


def gelu_grad(v):
    t = jnp.tanh(GELU_C * (v + GELU_A * (v * v * v)))
    return 0.5 * (1.0 + t) + (0.5 * GELU_C) * v * (1.0 - t * t) * (1.0 + (3 * GELU_A) * (v * v))


def dot_nt(a, b):
    return lax.dot_general(a, b, (((1,), (1,)), ((), ())), preferred_element_type=F32)


def dot_nn(a, b):
    return jnp.dot(a, b, preferred_element_type=F32)


def stream(layer, w_up, w_down, up_buf, down_buf, sem):
    def copies(c):
        buf = lax.rem(c, N_BUF)
        f = pl.multiple_of(c * FCH, FCH)
        return (pltpu.make_async_copy(w_up.at[layer, :, pl.ds(f, FCH)], up_buf.at[buf], sem.at[0, buf]),
                pltpu.make_async_copy(w_down.at[layer, pl.ds(f, FCH), :], down_buf.at[buf], sem.at[1, buf]))

    return copies


def forward_kernel(layer, keep, x_ref, u_ref, r0_ref, r1_ref, r2_ref, r3_ref, pick_ref, w_up, w_down, w_gate, w_proj, *rest):
    if keep:
        x_out, u_out, up_hbm, gate_hbm, got_out = rest[:5]
        up_buf, down_buf, gate_w, proj_w, acc, up_stage, gate_stage, sem, sem_gp, sem_o = rest[5:]
    else:
        x_out, u_out = rest[:2]
        up_buf, down_buf, gate_w, proj_w, acc, sem, sem_gp = rest[2:]
    n_ch = w_up.shape[2] // FCH
    copies = stream(layer, w_up, w_down, up_buf, down_buf, sem)
    for c in range(N_BUF - 1):
        for cp in copies(c):
            cp.start()
    gate_cp = pltpu.make_async_copy(w_gate.at[layer], gate_w, sem_gp.at[0])
    proj_cp = pltpu.make_async_copy(w_proj.at[layer], proj_w, sem_gp.at[1])
    gate_cp.start()
    proj_cp.start()

    def stage_copy(c):
        buf = lax.rem(c, 2)
        return pltpu.make_async_copy(
            up_stage.at[buf], up_hbm.at[:, pl.ds(pl.multiple_of(c * FCH, FCH), FCH)], sem_o.at[buf])

    acc[...] = x_ref[...].astype(F32)

    def chunk(c, _):
        @pl.when(c + N_BUF - 1 < n_ch)
        def _():
            for cp in copies(c + N_BUF - 1):
                cp.start()

        for cp in copies(c):
            cp.wait()
        if keep:
            @pl.when(c >= 2)
            def _():
                stage_copy(c - 2).wait()

        buf = lax.rem(c, N_BUF)
        hidden = []
        for n in range(FCH // 256):
            pre = dot_nn(u_ref[...], up_buf[buf, :, n * 256:(n + 1) * 256])
            if keep:
                up_stage[lax.rem(c, 2), :, n * 256:(n + 1) * 256] = pre
            hidden.append(jax.nn.gelu(pre).astype(BF))
        hidden = jnp.concatenate(hidden, axis=1)
        for n in range(4):
            acc[:, n * 256:(n + 1) * 256] += dot_nn(hidden, down_buf[buf, :, n * 256:(n + 1) * 256])
        if keep:
            stage_copy(c).start()
        return 0

    lax.fori_loop(0, n_ch, chunk, 0)
    gate_cp.wait()
    proj_cp.wait()
    mixed = []
    for n in range(4):
        cols = slice(n * 256, (n + 1) * 256)
        pre = dot_nn(u_ref[...], gate_w[:, cols])
        cap = r0_ref.shape[0]
        got = sum(dot_nn(pick_ref[:, f * cap:(f + 1) * cap], r[:, cols])
                  for f, r in enumerate((r0_ref, r1_ref, r2_ref, r3_ref))).astype(BF)
        if keep:
            gate_stage[:, cols] = pre
            got_out[:, cols] = got
        mixed.append((jax.nn.gelu(pre) * got.astype(F32)).astype(BF))
    mixed = jnp.concatenate(mixed, axis=1)
    if keep:
        gate_out = pltpu.make_async_copy(gate_stage, gate_hbm, sem_o.at[2])
        gate_out.start()
    for n in range(4):
        cols = slice(n * 256, (n + 1) * 256)
        x_out[:, cols] = (acc[:, cols] + dot_nn(mixed, proj_w[:, cols])).astype(BF)
    x_next = x_out[...].astype(F32)
    scale = lax.rsqrt(jnp.mean(x_next * x_next, axis=-1, keepdims=True) + NORM_EPS)
    u_out[...] = (x_next * scale).astype(BF)
    if keep:
        gate_out.wait()
        stage_copy(n_ch - 2).wait()
        stage_copy(n_ch - 1).wait()


def layer_fwd(layer, keep, x, u, rows, pick, w_up, w_down, w_gate, w_proj):
    t, d = x.shape
    f = w_up.shape[2]
    hbm = pl.BlockSpec(memory_space=pltpu.HBM)
    vmem = pl.BlockSpec(memory_space=pltpu.VMEM)
    act = jax.ShapeDtypeStruct((t, d), BF)
    out_shape = [act, act]
    out_specs = [vmem, vmem]
    scratch = [
        pltpu.VMEM((N_BUF, d, FCH), BF), pltpu.VMEM((N_BUF, FCH, d), BF),
        pltpu.VMEM((d, d), BF), pltpu.VMEM((d, d), BF), pltpu.VMEM((t, d), F32),
    ]
    sems = [pltpu.SemaphoreType.DMA((2, N_BUF)), pltpu.SemaphoreType.DMA((2,))]
    if keep:
        out_shape += [pltpu.HBM((t, f), F32), pltpu.HBM((t, d), F32), act]
        out_specs += [hbm, hbm, vmem]
        scratch += [pltpu.VMEM((2, t, FCH), F32), pltpu.VMEM((t, d), F32)]
        sems += [pltpu.SemaphoreType.DMA((3,))]
    return pl.pallas_call(
        functools.partial(forward_kernel, layer, keep),
        out_shape=out_shape, in_specs=[vmem] * 7 + [hbm] * 4, out_specs=out_specs,
        scratch_shapes=scratch + sems,
        compiler_params=pltpu.CompilerParams(vmem_limit_bytes=40 << 20),
        cost_estimate=pl.CostEstimate(flops=11_000_000_000, bytes_accessed=30_000_000, transcendentals=0),
    )(x, u, *rows, pick, *in_hbm(w_up, w_down, w_gate, w_proj))


def backward_kernel(layer, cot_ref, dm_ref, x_ref, got_ref, up_hbm, gate_hbm, w_up, w_down, w_gate, w_proj,
                    cot_out, dm_out, up_buf, down_buf, pre_buf, gate_w, proj_w, gate_pre, acc, sem, sem_gp):
    n_ch = w_up.shape[2] // FCH
    copies = stream(layer, w_up, w_down, up_buf, down_buf, sem)

    def all_copies(c):
        buf = lax.rem(c, N_BUF)
        pre = pltpu.make_async_copy(
            up_hbm.at[:, pl.ds(pl.multiple_of(c * FCH, FCH), FCH)], pre_buf.at[buf], sem.at[2, buf])
        return copies(c) + (pre,)

    for c in range(N_BUF - 1):
        for cp in all_copies(c):
            cp.start()
    gate_cp = pltpu.make_async_copy(w_gate.at[layer], gate_w, sem_gp.at[0])
    pre_cp = pltpu.make_async_copy(gate_hbm, gate_pre, sem_gp.at[1])
    proj_cp = pltpu.make_async_copy(w_proj.at[layer - 1], proj_w, sem_gp.at[2])
    for cp in (gate_cp, pre_cp, proj_cp):
        cp.start()

    def chunk(c, _):
        @pl.when(c + N_BUF - 1 < n_ch)
        def _():
            for cp in all_copies(c + N_BUF - 1):
                cp.start()

        for cp in all_copies(c):
            cp.wait()
        buf = lax.rem(c, N_BUF)
        d_pre = []
        for n in range(FCH // 256):
            cols = slice(n * 256, (n + 1) * 256)
            d_hidden = dot_nt(cot_ref[...], down_buf[buf, cols, :]).astype(BF).astype(F32)
            d_pre.append((d_hidden * gelu_grad(pre_buf[buf, :, cols])).astype(BF))
        d_pre = jnp.concatenate(d_pre, axis=1)
        for n in range(4):
            cols = slice(n * 256, (n + 1) * 256)
            part = dot_nt(d_pre, up_buf[buf, cols, :])
            acc[:, cols] = part + jnp.where(c == 0, 0.0, acc[:, cols])
        return 0

    lax.fori_loop(0, n_ch, chunk, 0)
    for cp in (gate_cp, pre_cp, proj_cp):
        cp.wait()
    d_pre = []
    for n in range(4):
        cols = slice(n * 256, (n + 1) * 256)
        d_act = dm_ref[:, cols].astype(F32) * got_ref[:, cols].astype(F32)
        d_pre.append((d_act * gelu_grad(gate_pre[:, cols])).astype(BF))
    d_pre = jnp.concatenate(d_pre, axis=1)
    for n in range(4):
        cols = slice(n * 256, (n + 1) * 256)
        both = acc[:, cols].astype(BF) + dot_nt(d_pre, gate_w[cols, :]).astype(BF)
        acc[:, cols] = both.astype(F32)
    x = x_ref[...].astype(F32)
    dy = acc[...]
    r = lax.rsqrt(jnp.mean(x * x, axis=-1, keepdims=True) + NORM_EPS)
    proj = jnp.mean(x * dy, axis=-1, keepdims=True)
    cot = (cot_ref[...].astype(F32) + (dy * r - x * (r * r * r * proj))).astype(BF)
    cot_out[...] = cot
    for n in range(4):
        cols = slice(n * 256, (n + 1) * 256)
        dm_out[:, cols] = dot_nt(cot, proj_w[cols, :]).astype(BF)


def layer_bwd(layer, cot, d_mixed, x, got, up_pre, gate_pre, w_up, w_down, w_gate, w_proj):
    t, d = x.shape
    hbm = pl.BlockSpec(memory_space=pltpu.HBM)
    vmem = pl.BlockSpec(memory_space=pltpu.VMEM)
    act = jax.ShapeDtypeStruct((t, d), BF)
    return pl.pallas_call(
        functools.partial(backward_kernel, layer),
        out_shape=[act, act], in_specs=[vmem] * 4 + [hbm] * 6, out_specs=[vmem, vmem],
        scratch_shapes=[
            pltpu.VMEM((N_BUF, d, FCH), BF), pltpu.VMEM((N_BUF, FCH, d), BF), pltpu.VMEM((N_BUF, t, FCH), F32),
            pltpu.VMEM((d, d), BF), pltpu.VMEM((d, d), BF), pltpu.VMEM((t, d), F32), pltpu.VMEM((t, d), F32),
            pltpu.SemaphoreType.DMA((3, N_BUF)), pltpu.SemaphoreType.DMA((3,)),
        ],
        compiler_params=pltpu.CompilerParams(vmem_limit_bytes=40 << 20),
        cost_estimate=pl.CostEstimate(flops=11_000_000_000, bytes_accessed=40_000_000, transcendentals=0),
    )(cot, d_mixed, x, got, *in_hbm(up_pre, gate_pre, w_up, w_down, w_gate, w_proj))


PICK = 32


def serve_kernel(n_layers, cap, cnt_ref, start_ref, ids_ref, pick_ref, tables, *rest):
    blocks, sem = rest[-2:]
    n_emb = len(rest[:-2]) // n_layers
    range_rows = tables.shape[1]

    def issue(e):
        def body(s, _):
            row = lax.rem(ids_ref[start_ref[e] + s], range_rows)
            row = pl.multiple_of(lax.div(row, 8) * 8, 8)
            slot = pl.multiple_of(s * 8, 8)
            pltpu.make_async_copy(
                tables.at[:, pl.ds(row, 8), :], blocks.at[e % 2, :, pl.ds(slot, 8), :], sem.at[e % 2]).start()
            return 0

        lax.fori_loop(0, cnt_ref[e] * PICK, body, 0)

    issue(0)
    for e in range(n_emb):
        buf = e % 2
        if e + 1 < n_emb:
            issue(e + 1)

        def drain(s, _):
            pltpu.make_async_copy(
                tables.at[:, pl.ds(0, 8 * PICK), :], blocks.at[buf, :, pl.ds(0, 8 * PICK), :], sem.at[buf]).wait()
            return 0

        lax.fori_loop(0, cnt_ref[e], drain, 0)

        def take(b, _):
            r = pl.multiple_of(b * PICK, PICK)
            pick = pick_ref[pl.ds(pl.multiple_of(e * cap + r, PICK), PICK), :]
            for l in range(n_layers):
                rows = blocks[buf, l, pl.ds(pl.multiple_of(r * 8, 8 * PICK), 8 * PICK), :]
                rest[l * n_emb + e][pl.ds(r, PICK), :] = jnp.dot(pick, rows, preferred_element_type=F32).astype(BF)
            return 0

        lax.fori_loop(0, cnt_ref[e], take, 0)

        def blank(b, _):
            r = pl.multiple_of(b * PICK, PICK)
            for l in range(n_layers):
                rest[l * n_emb + e][pl.ds(r, PICK), :] = jnp.zeros((PICK, tables.shape[2]), BF)
            return 0

        lax.fori_loop(cnt_ref[e], cap // PICK, blank, 0)


def serve_rows(tables, counts, starts, ids, pick, cap):
    n_layers, _, width = tables.shape
    n_emb = counts.shape[0]
    smem = pl.BlockSpec(memory_space=pltpu.SMEM)
    vmem = pl.BlockSpec(memory_space=pltpu.VMEM)
    return pl.pallas_call(
        functools.partial(serve_kernel, n_layers, cap),
        out_shape=[jax.ShapeDtypeStruct((cap, width), BF)] * (n_layers * n_emb),
        in_specs=[smem, smem, smem, vmem, pl.BlockSpec(memory_space=pltpu.HBM)],
        out_specs=[vmem] * (n_layers * n_emb),
        scratch_shapes=[
            pltpu.VMEM((2, n_layers, cap * 8, width), BF),
            pltpu.SemaphoreType.DMA((2,)),
        ],
        compiler_params=pltpu.CompilerParams(vmem_limit_bytes=48 << 20),
        cost_estimate=pl.CostEstimate(flops=20_000_000_000, bytes_accessed=30_000_000, transcendentals=0),
        name="serve_rows",
    )(counts, starts, ids, pick, *in_hbm(tables))


N_SRC = 16
MAX_ROWS = 17 * BLK


def pull_runs(meta_ref, srcs, dst, sem):

    def run(src, k, base):
        lo, off = meta_ref[k], meta_ref[2 * N_SRC + k]

        def chunk(c, _):
            a = pl.multiple_of(base + lo + c * CHUNK, CHUNK)
            b = pl.multiple_of((off + c) * CHUNK, CHUNK)
            pltpu.make_async_copy(src.at[pl.ds(a, CHUNK), :], dst.at[pl.ds(b, CHUNK), :], sem).start()
            return 0

        lax.fori_loop(0, meta_ref[N_SRC + k], chunk, 0)

    if len(srcs) == 1:
        src_rows = srcs[0].shape[0] // N_SRC
        lax.fori_loop(0, N_SRC, lambda k, c: (run(srcs[0], k, k * src_rows), c)[1], 0)
    else:
        for j, src in enumerate(srcs):
            run(src, meta_ref[3 * N_SRC + 1 + j], 0)


def drain_runs(meta_ref, srcs, dst, sem):
    def one(c, _):
        pltpu.make_async_copy(srcs[0].at[pl.ds(0, CHUNK), :], dst.at[pl.ds(0, CHUNK), :], sem).wait()
        return 0

    lax.fori_loop(0, meta_ref[3 * N_SRC], one, 0)


def n_blocks(meta_ref):
    return lax.div(meta_ref[3 * N_SRC] * CHUNK + BLK - 1, BLK)


def gate_kernel(layer, meta_ref, w_ref, *rest):
    u_hbm, (out, uc, stage, sem_u, sem_o) = rest[:-5], rest[-5:]
    pull_runs(meta_ref, u_hbm, uc, sem_u)
    drain_runs(meta_ref, u_hbm, uc, sem_u)
    total = n_blocks(meta_ref)

    def out_copy(b):
        buf = lax.rem(b, 2)
        return pltpu.make_async_copy(stage.at[buf], out.at[pl.ds(b * (BLK // 8), BLK // 8)], sem_o.at[buf])

    def block(b, _):
        @pl.when(b >= 2)
        def _():
            out_copy(b - 2).wait()

        u = uc[pl.ds(pl.multiple_of(b * BLK, BLK), BLK), :]
        for n in range(4):
            pre = jnp.dot(u, w_ref[layer, :, n * 256:(n + 1) * 256], preferred_element_type=F32)
            act = jax.nn.gelu(pre)
            for j in range(2):
                stage[lax.rem(b, 2), :, n * 2 + j] = act[:, j * 128:(j + 1) * 128].reshape(BLK // 8, 8, 128)
        out_copy(b).start()
        return 0

    lax.fori_loop(0, total, block, 0)
    lax.fori_loop(jnp.maximum(total - 2, 0), total, lambda b, c: (out_copy(b).wait(), c)[1], 0)


def owner_gate(layer, meta, u_all, w_gate):
    smem = pl.BlockSpec(memory_space=pltpu.SMEM)
    hbm = pl.BlockSpec(memory_space=pltpu.HBM)
    width = w_gate.shape[2]
    return pl.pallas_call(
        functools.partial(gate_kernel, layer),
        out_shape=pltpu.HBM((MAX_ROWS // 8, width // 128, 8, 128), F32),
        in_specs=[smem, pl.BlockSpec(memory_space=pltpu.VMEM)] + [hbm] * len(u_all),
        out_specs=hbm,
        scratch_shapes=[
            pltpu.VMEM((MAX_ROWS, width), BF),
            pltpu.VMEM((2, BLK // 8, width // 128, 8, 128), F32),
            pltpu.SemaphoreType.DMA,
            pltpu.SemaphoreType.DMA((2,)),
        ],
        compiler_params=pltpu.CompilerParams(vmem_limit_bytes=28 << 20),
        cost_estimate=pl.CostEstimate(flops=10_000_000_000, bytes_accessed=30_000_000, transcendentals=0),
    )(meta, w_gate, *in_hbm(*u_all))


UNROLL = 8


def owner_kernel(layer, n_src, meta_ref, tile_ref, addr_ref, g_hbm, *rest):
    d_hbm = rest[:n_src]
    out, dc, prod, acc, sem_d, sem_g, sem_o = rest[-7:]
    n_tiles = tile_ref.shape[0] - 1
    total = n_blocks(meta_ref)

    def g_copy(b):
        n = BLK // 8
        return pltpu.make_async_copy(
            g_hbm.at[pl.ds(b * n, n)], prod.reshape(MAX_ROWS // 8, 8, 8, 128).at[pl.ds(b * n, n)], sem_g.at[b])

    pull_runs(meta_ref, d_hbm, dc, sem_d)
    lax.fori_loop(0, total, lambda b, c: (g_copy(b).start(), c)[1], 0)

    def clear(buf):
        def some(i, _):
            acc[buf, pl.ds(pl.multiple_of(i * 512, 512), 512), :] = jnp.zeros((512, 128), F32)
            return 0

        lax.fori_loop(0, TILE_ROWS * 8 // 512, some, 0)

    clear(0)
    clear(1)
    drain_runs(meta_ref, d_hbm, dc, sem_d)

    def block(b, _):
        g_copy(b).wait()
        for t in range(BLK // 16):
            d = dc[pl.ds(pl.multiple_of(b * BLK + t * 16, 16), 16), :].astype(F32)
            for h in range(2):
                for j in range(8):
                    at = pl.ds(pl.multiple_of(b * (BLK * 8) + (2 * t + h) * 64 + j * 8, 8), 8)
                    prod[at, :] = prod[at, :] * d[h * 8:(h + 1) * 8, j * 128:(j + 1) * 128]
        return 0

    lax.fori_loop(0, total, block, 0)

    def out_copy(t, buf):
        return pltpu.make_async_copy(
            acc.at[buf].reshape(TILE_ROWS // 8, 8, 8, 128),
            out.at[layer, pl.ds(t * (TILE_ROWS // 8), TILE_ROWS // 8)], sem_o.at[buf])

    def tile(t, _):
        buf = lax.rem(t, 2)

        @pl.when(t >= 2)
        def _():
            out_copy(t - 2, buf).wait()
            clear(buf)

        first, last = tile_ref[t], tile_ref[t + 1]

        def one(i, run):
            word = addr_ref[i]
            pa = lax.bitwise_and(word, 0xFFFF)
            ra = lax.bitwise_and(lax.shift_right_logical(word, 16), 0x1FFF)
            fresh = word >= (1 << 29)
            run = jnp.where(fresh, 0.0, run) + prod[pl.ds(pa, 8, stride=8), :]
            acc[buf, pl.ds(ra, 8, stride=8), :] = run
            return run

        def many(i, run):
            for u in range(UNROLL):
                run = one(first + i * UNROLL + u, run)
            return run

        groups = lax.div(last - first, UNROLL)
        run = lax.fori_loop(0, groups, many, jnp.zeros((8, 128), F32))
        lax.fori_loop(first + groups * UNROLL, last, one, run)
        out_copy(t, buf).start()
        return 0

    lax.fori_loop(0, n_tiles, tile, 0)
    out_copy(n_tiles - 2, n_tiles % 2).wait()
    out_copy(n_tiles - 1, (n_tiles - 1) % 2).wait()


def owner_grad(layer, out_prev, out_shape, meta, tiles, addrs, g_rows, d_all):
    smem = pl.BlockSpec(memory_space=pltpu.SMEM)
    hbm = pl.BlockSpec(memory_space=pltpu.HBM)
    width = g_rows.shape[1] * 128
    args = [meta, tiles, addrs, *in_hbm(g_rows, *d_all)]
    specs = [smem, smem, smem, hbm] + [hbm] * len(d_all)
    aliases = {}
    if out_prev is not None:
        args.append(out_prev)
        specs.append(hbm)
        aliases = {len(args) - 1: 0}
    return pl.pallas_call(
        functools.partial(owner_kernel, layer, len(d_all)),
        out_shape=jax.ShapeDtypeStruct(out_shape, F32),
        in_specs=specs,
        out_specs=hbm,
        scratch_shapes=[
            pltpu.VMEM((MAX_ROWS, width), BF),
            pltpu.VMEM((MAX_ROWS * 8, 128), F32),
            pltpu.VMEM((2, TILE_ROWS * 8, 128), F32),
            pltpu.SemaphoreType.DMA,
            pltpu.SemaphoreType.DMA((MAX_ROWS // BLK,)),
            pltpu.SemaphoreType.DMA((2,)),
        ],
        input_output_aliases=aliases,
        compiler_params=pltpu.CompilerParams(vmem_limit_bytes=48 << 20),
        cost_estimate=pl.CostEstimate(flops=40_000_000_000, bytes_accessed=100_000_000, transcendentals=0),
    )(*args)


def solution(mesh):
    n_emb = mesh.shape['emb']
    n_dev = n_emb * mesh.shape['dp']
    tok_spec = P(('dp', 'emb'))
    act_spec = P(('dp', 'emb'), None)
    table_spec = P(None, 'emb', None)
    full_spec = P(None, None, None)
    everyone = ('dp', 'emb')

    def device_body(tok_ids, resid_in, cot_out, tables, w_up, w_down, w_gate, w_proj):
        n_layers, range_rows, width = tables.shape
        n_dp = n_dev // n_emb
        n_tok = tok_ids.shape[0]
        cap = min(2 * n_tok // n_emb, 3 * n_tok // 4)
        i_dp, i_emb = lax.axis_index('dp'), lax.axis_index('emb')
        last = n_layers - 1

        def gather(rows):
            return lax.all_gather(rows, everyone, axis=0, tiled=True)

        pos = jnp.arange(n_tok, dtype=jnp.int32)
        before = (tok_ids[None, :] < tok_ids[:, None]) | ((tok_ids[None, :] == tok_ids[:, None]) & (pos[None, :] < pos[:, None]))
        rank = jnp.sum(before.astype(jnp.int32), axis=1)
        perm_mask = rank[None, :] == pos[:, None]
        perm = perm_mask.astype(BF)
        x = jnp.dot(perm, resid_in, preferred_element_type=F32).astype(BF)
        normed = rms_norm(x.astype(F32)).astype(BF)
        u_sets = [[gather(normed)]]

        def flip(block, axis, bit):
            n = mesh.shape[axis]
            return lax.ppermute(block, axis, [(i, i ^ bit) for i in range(n)])

        def spread(block, x_heavy):
            at = {(0, 0, 0): block}
            at[1, 0, 0] = flip(block, 'emb', 2)
            at[0, 1, 0] = flip(block, 'dp', 1)
            at[0, 0, 1] = flip(block, 'dp', 2)
            at[0, 1, 1] = flip(at[0, 1, 0], 'dp', 2)
            if x_heavy:
                at[1, 0, 1] = flip(at[0, 0, 1], 'emb', 2)
                at[1, 1, 0] = flip(at[0, 1, 0], 'emb', 2)
            else:
                at[1, 0, 1] = flip(at[1, 0, 0], 'dp', 2)
                at[1, 1, 0] = flip(at[1, 0, 0], 'dp', 1)
            at[1, 1, 1] = flip(at[1, 0, 1], 'dp', 1)
            offsets = sorted(at, key=lambda o: (sum(o), o))
            blocks = [at[o] for o in offsets] + [flip(at[o], 'emb', 1) for o in offsets]
            places = [((o[2] * 2 + o[1]), (o[0] * 2 + c)) for c in range(2) for o in offsets]
            return blocks, places

        ids = jnp.sum(jnp.where(perm_mask, tok_ids[None, :], 0), axis=1)
        ids, _ = lax.optimization_barrier((ids, normed))
        ids_all = share_ids(ids, n_dp, n_emb)
        ids_2d = ids_all.reshape(n_dev, n_tok)
        base = i_emb * range_rows

        peers = i_dp * n_emb + (i_emb ^ jnp.arange(n_emb, dtype=jnp.int32))
        is_peer = peers[:, None] == jnp.arange(n_dev, dtype=jnp.int32)[None, :]
        mine = jnp.sum(jnp.where(is_peer[:, :, None], ids_2d[None], 0), axis=1)
        peer_lo = jnp.sum((mine < base).astype(jnp.int32), axis=1)
        count = jnp.sum((mine < base + range_rows).astype(jnp.int32), axis=1) - peer_lo
        slot_pos = jnp.arange(cap, dtype=jnp.int32)
        at = pos[None, None, :] == (peer_lo[:, None] + slot_pos[None, :])[:, :, None]
        low = jnp.sum(jnp.where(at, mine[:, None, :] % 8, 0), axis=2)
        pick_col = jnp.where(slot_pos[None, :] < count[:, None], (slot_pos[None, :] % PICK) * 8 + low, -1)
        pick8 = (pick_col.reshape(-1, 1) == jnp.arange(8 * PICK, dtype=jnp.int32)[None, :]).astype(BF)
        served = serve_rows(tables, (count + PICK - 1) // PICK, peer_lo + peers * n_tok,
                            jnp.pad(ids_all, (0, PICK)), pick8, cap)
        returned = [[served[l * n_emb]] + [flip(served[l * n_emb + f], 'emb', f) for f in range(1, n_emb)]
                    for l in range(n_layers)]
        owner = ids // range_rows
        first = jnp.sum((owner[None, :] < owner[:, None]).astype(jnp.int32), axis=1)
        slot = (owner ^ i_emb) * cap + pos - first
        pick = (slot[:, None] == jnp.arange(n_emb * cap, dtype=jnp.int32)[None, :]).astype(BF)

        cot_in, _ = lax.optimization_barrier((cot_out, served[0]))
        cot = jnp.dot(perm, cot_in, preferred_element_type=F32).astype(BF)
        d_mixed = lax.dot_general(cot, w_proj[last], (((1,), (1,)), ((), ())), preferred_element_type=F32).astype(BF)
        d_sets = [None] * n_layers
        d_sets[last], places = spread(d_mixed, False)
        sources = jnp.stack([(i_dp ^ d) * n_emb + (i_emb ^ e) for d, e in places]).astype(jnp.int32)

        n_tiles = range_rows // TILE_ROWS
        lo = jnp.sum((ids_2d < base).astype(jnp.int32), axis=1)
        hi = jnp.sum((ids_2d < base + range_rows).astype(jnp.int32), axis=1)
        lo16 = (lo // CHUNK) * CHUNK
        n_ch = (hi - lo16 + CHUNK - 1) // CHUNK
        tri = jnp.arange(n_dev)[None, :] < jnp.arange(n_dev)[:, None]
        off = jnp.sum(jnp.where(tri, n_ch[None, :], 0), axis=1)
        meta = jnp.concatenate([lo16, n_ch, off, jnp.sum(n_ch)[None], sources]).astype(jnp.int32)
        place = (off * CHUNK - lo16)[:, None] + pos[None, :]
        local = ids_2d - base
        owned = (local >= 0) & (local < range_rows)
        key = jnp.where(owned, local * (1 << 13) + place, jnp.iinfo(jnp.int32).max)
        key = lax.sort(key.reshape(-1), is_stable=False)[:n_emb * n_dev * cap // 4]
        p, r = key & ((1 << 13) - 1), key >> 13
        fresh = jnp.concatenate([jnp.ones((1,), jnp.bool_), r[1:] != r[:-1]])
        in_tile = r % TILE_ROWS
        addrs = ((p // 8) * 64 + p % 8) | (((in_tile // 8) * 64 + in_tile % 8) << 16) | (fresh.astype(jnp.int32) << 29)
        edges = jnp.arange(n_tiles + 1, dtype=jnp.int32) * TILE_ROWS
        tiles = jnp.sum((r[None, :] < edges[:, None]).astype(jnp.int32), axis=1)

        pick, meta, tiles, addrs = lax.optimization_barrier((pick, meta, tiles, addrs))

        weights = (w_up, w_down, w_gate, w_proj)
        saved, u = [], normed
        for l in range(n_layers):
            x_in = x
            x, u, *kept = layer_fwd(l, l > 0, x, u, returned[l], pick, *weights)
            saved.append((x_in, *kept))
            if l < last:
                u_sets.append(spread(u, False)[0] if l == 0 else [gather(u)])
        resid_out = lax.dot_general(perm, x, (((0,), (0,)), ((), ())), preferred_element_type=F32).astype(BF)
        for l in range(last, 0, -1):
            x_in, up_pre, gate_pre, got = saved[l]
            cot, d_mixed = layer_bwd(l, cot, d_mixed, x_in, got, up_pre, gate_pre, *weights)
            d_sets[l - 1] = [gather(d_mixed)]

        u_sets[0][0], _ = lax.optimization_barrier((u_sets[0][0], d_mixed))
        grads = None
        out_shape = (n_layers, range_rows // 8, width // 128, 8, 128)
        gates = []
        for l in range(n_layers):
            gates.append(owner_gate(l, meta, u_sets[l], w_gate))
        for l in range(last, -1, -1):
            grads = owner_grad(l, grads, out_shape, meta, tiles, addrs, gates[l], d_sets[l])
        d_tables = grads.transpose(0, 1, 3, 2, 4).reshape(n_layers, range_rows, width)
        return resid_out, d_tables

    return jax.shard_map(device_body, mesh=mesh, in_specs=(tok_spec, act_spec, act_spec, table_spec, full_spec, full_spec, full_spec, full_spec), out_specs=(act_spec, table_spec), check_vma=False)
```
